32 devices in a mesh: dp: 2 (over x), tp: 4 (over z), sp: 4 (over y, core).
Axes of the slice: x: 2, y: 2, z: 4, core: 2. Of those that a mesh axis runs over, the one named last changes fastest.
Arguments:
- hidden: bfloat16 [32, 4096], P('dp'), parts along dimension 0
- positions: int32 [32], P('dp'), parts along dimension 0
- norm_attn: float32 [4096], replicated
- norm_mlp: float32 [4096], replicated
- w_qkv: bfloat16 [4096, 6144], P(None, 'tp')
- w_out: bfloat16 [4096, 4096], P('tp')
- w_gate_up: bfloat16 [4096, 28672], P(None, 'tp')
- w_down: bfloat16 [14336, 4096], P('tp')
- k_cache: bfloat16 [32, 4096, 8, 128], P('dp', 'sp', 'tp'), parts along dimension 0
- v_cache: bfloat16 [32, 4096, 8, 128], P('dp', 'sp', 'tp'), parts along dimension 0
Outputs:
- output 1: bfloat16 [32, 4096], P('dp'), parts along dimension 0
- output 2: bfloat16 [32, 4096, 8, 128], P('dp', 'sp', 'tp'), parts along dimension 0
- output 3: bfloat16 [32, 4096, 8, 128], P('dp', 'sp', 'tp'), parts along dimension 0
There are 2 independent parts. The reference program is written for one: setup_inputs(seed, part) draws one part's arguments, and reference() takes and returns one part's arrays. A program takes and returns all parts, laid end to end along the dimension named above; an argument that names none is the same for every part.
All inputs are finite; a program needn't handle non-finite values.
Results may differ from the reference program's by a relative error of at most 0.00869568.
Values sent between devices are 32-bit elements.
A program may use at most 1 GiB of HBM per device.

```python
import jax
import jax.numpy as jnp
from jax import lax

NUM_SEQS = 16
CACHE_LEN = 4096
TEN_PAR = 4
MODEL_DIM = 4096
NUM_HEADS = 32
KV_HEADS = 8
HEAD_DIM = 128
FFN_DIM = 14336
WINDOW = 2047

GROUP_SIZE = NUM_HEADS // KV_HEADS
QKV_COLS = (NUM_HEADS + 2 * KV_HEADS) * HEAD_DIM
FFN_LOCAL = FFN_DIM // TEN_PAR
ROPE_BASE = 10000.0
NORM_EPS = 1e-5


def rms_norm(values, gain_vec):
    mean_sq = jnp.mean(values * values, axis=-1, keepdims=True)
    return values * lax.rsqrt(mean_sq + NORM_EPS) * gain_vec


def rope_angles(positions):
    inv_freq = ROPE_BASE ** (-jnp.arange(0, HEAD_DIM, 2).astype(jnp.float32) / HEAD_DIM)
    angles = positions.astype(jnp.float32)[:, None] * inv_freq[None, :]
    angles = jnp.concatenate([angles, angles], axis=-1)
    return jnp.cos(angles), jnp.sin(angles)


def rotate_half(values, cos_tab, sin_tab):
    half_dim = values.shape[-1] // 2
    turned = jnp.concatenate([-values[..., half_dim:], values[..., :half_dim]], axis=-1)
    return values * cos_tab + turned * sin_tab


def seq_attention(operands):
    q_rows, k_seq, v_seq, position = operands
    scores = jnp.einsum('kgd,jkd->kgj', q_rows.astype(jnp.float32), k_seq.astype(jnp.float32)) * (HEAD_DIM ** -0.5)
    slot_ids = jnp.arange(CACHE_LEN)
    in_window = (slot_ids <= position) & (slot_ids >= position - WINDOW)
    scores = jnp.where(in_window, scores, -jnp.inf)
    row_max = jnp.max(scores, axis=-1, keepdims=True)
    weights = jnp.exp(scores - row_max)
    weight_sum = jnp.sum(weights, axis=-1)
    acc_sum = jnp.einsum('kgj,jkd->kgd', weights.astype(jnp.bfloat16).astype(jnp.float32), v_seq.astype(jnp.float32))
    return (acc_sum / weight_sum[..., None]).astype(jnp.bfloat16)


def setup_inputs(seed: int = 0, part: int = 0) -> dict:
    base_key = jax.random.key(seed)
    shared_keys = jax.random.split(base_key, 6)
    own_keys = jax.random.split(jax.random.fold_in(base_key, part), 6)
    cache_shape = (NUM_SEQS, CACHE_LEN, KV_HEADS, HEAD_DIM)
    hidden = jax.random.normal(own_keys[0], (NUM_SEQS, MODEL_DIM), jnp.float32).astype(jnp.bfloat16)
    low_pos = WINDOW // 2
    drawn_pos = jax.random.randint(own_keys[1], (NUM_SEQS,), low_pos, CACHE_LEN, jnp.int32)
    row_ids = jnp.arange(NUM_SEQS)
    positions = jnp.where(row_ids == 0, CACHE_LEN - 1, drawn_pos)
    positions = jnp.where(jnp.logical_and(row_ids == NUM_SEQS - 1, NUM_SEQS > 1), low_pos, positions).astype(jnp.int32)
    norm_attn = 1.0 + 0.3 * jax.random.normal(shared_keys[0], (MODEL_DIM,), jnp.float32)
    norm_mlp = 1.0 + 0.3 * jax.random.normal(shared_keys[1], (MODEL_DIM,), jnp.float32)
    w_qkv = (jax.random.normal(shared_keys[2], (MODEL_DIM, QKV_COLS), jnp.float32) * MODEL_DIM ** -0.5).astype(jnp.bfloat16)
    w_out = (jax.random.normal(shared_keys[3], (NUM_HEADS * HEAD_DIM, MODEL_DIM), jnp.float32) * (NUM_HEADS * HEAD_DIM) ** -0.5).astype(jnp.bfloat16)
    w_gate_up = (jax.random.normal(shared_keys[4], (MODEL_DIM, 2 * FFN_DIM), jnp.float32) * MODEL_DIM ** -0.5).astype(jnp.bfloat16)
    w_down = (jax.random.normal(shared_keys[5], (FFN_DIM, MODEL_DIM), jnp.float32) * FFN_DIM ** -0.5).astype(jnp.bfloat16)
    pos_wave = jnp.cos(jnp.pi * jnp.arange(CACHE_LEN).astype(jnp.float32) / WINDOW)[None, :, None, None]
    key_dir = jax.random.normal(own_keys[3], (NUM_SEQS, 1, KV_HEADS, HEAD_DIM), jnp.float32)
    k_cache = (jax.random.normal(own_keys[2], cache_shape, jnp.float32) + key_dir * pos_wave).astype(jnp.bfloat16)
    v_trend = 2.0 * jax.random.normal(own_keys[5], (NUM_SEQS, 1, KV_HEADS, HEAD_DIM), jnp.float32)
    v_cache = (jax.random.normal(own_keys[4], cache_shape, jnp.float32) + v_trend * pos_wave).astype(jnp.bfloat16)
    return {'hidden': hidden, 'positions': positions, 'norm_attn': norm_attn, 'norm_mlp': norm_mlp, 'w_qkv': w_qkv, 'w_out': w_out, 'w_gate_up': w_gate_up, 'w_down': w_down, 'k_cache': k_cache, 'v_cache': v_cache}


def reference(hidden, positions, norm_attn, norm_mlp, w_qkv, w_out, w_gate_up, w_down, k_cache, v_cache):
    num_rows = hidden.shape[0]
    resid_in = hidden.astype(jnp.float32)
    normed = rms_norm(resid_in, norm_attn).astype(jnp.bfloat16)
    qkv_proj = jnp.dot(normed, w_qkv, preferred_element_type=jnp.float32).reshape(num_rows, KV_HEADS, GROUP_SIZE + 2, HEAD_DIM)
    cos_tab, sin_tab = rope_angles(positions)
    q_new = rotate_half(qkv_proj[:, :, :GROUP_SIZE], cos_tab[:, None, None], sin_tab[:, None, None]).astype(jnp.bfloat16)
    k_new = rotate_half(qkv_proj[:, :, GROUP_SIZE], cos_tab[:, None], sin_tab[:, None]).astype(jnp.bfloat16)
    v_new = qkv_proj[:, :, GROUP_SIZE + 1].astype(jnp.bfloat16)
    slot_ids = jnp.arange(CACHE_LEN)
    at_slot = (slot_ids[None, :] == positions[:, None])[:, :, None, None]
    k_upd = jnp.where(at_slot, k_new[:, None], k_cache)
    v_upd = jnp.where(at_slot, v_new[:, None], v_cache)
    attended = lax.map(seq_attention, (q_new, k_upd, v_upd, positions)).reshape(num_rows, NUM_HEADS * HEAD_DIM)
    out_parts = jnp.einsum('bsk,skd->bsd', attended.reshape(num_rows, TEN_PAR, -1).astype(jnp.float32), w_out.reshape(TEN_PAR, -1, MODEL_DIM).astype(jnp.float32))
    mid_resid = resid_in + jnp.sum(out_parts.astype(jnp.bfloat16).astype(jnp.float32), axis=1)
    normed_mlp = rms_norm(mid_resid, norm_mlp).astype(jnp.bfloat16)
    gate_up = jnp.dot(normed_mlp, w_gate_up, preferred_element_type=jnp.float32).reshape(num_rows, TEN_PAR, 2, FFN_LOCAL)
    act_vals = (jax.nn.silu(gate_up[:, :, 0]) * gate_up[:, :, 1]).astype(jnp.bfloat16)
    down_parts = jnp.einsum('bsf,sfd->bsd', act_vals.astype(jnp.float32), w_down.reshape(TEN_PAR, FFN_LOCAL, MODEL_DIM).astype(jnp.float32))
    result = mid_resid + jnp.sum(down_parts.astype(jnp.bfloat16).astype(jnp.float32), axis=1)
    return (result.astype(jnp.bfloat16), k_upd, v_upd)
```

```python
import functools

import jax
import jax.numpy as jnp
from jax import lax
from jax.experimental import pallas as pl
from jax.experimental.pallas import tpu as pltpu
from jax.sharding import PartitionSpec as P

WINDOW = 2047
ROPE_BASE = 10000.0
NORM_EPS = 1e-5
MESH = pl.DeviceIdType.MESH
F32 = jnp.float32
BF16 = jnp.bfloat16
NEG = float(jnp.finfo(jnp.float32).min)

TP = 4
SP = 4
W_CHUNKS = 8
GROUP = 4
OFFSETS = (
    (0, 1), (0, 2), (0, 3), (1, 0), (1, 1), (2, 0), (2, 1), (1, 2), (1, 3),
    (3, 0), (3, 1), (2, 2), (2, 3), (3, 2), (3, 3),
)


def rope_tables(positions, head_dim):
    inv_freq = ROPE_BASE ** (-jnp.arange(0, head_dim, 2).astype(F32) / head_dim)
    angles = positions.astype(F32)[:, None] * inv_freq[None, :]
    cos, sin = jnp.cos(angles), jnp.sin(angles)
    return jnp.concatenate([cos, cos], axis=-1), jnp.concatenate([-sin, sin], axis=-1)


def attend_kernel(
    ploc_ref, x_ref, gain_ref, cos_ref, sin_ref, wq_ref, k_ref, v_ref,
    k_out, v_out, part_ref,
    k_buf, v_buf, w_buf, r_buf, q_buf, kn_buf, vn_buf, w_sem, k_sem, v_sem, ko_sem, vo_sem,
):
    rows, dim = x_ref.shape
    keys = k_ref.shape[1]
    depth = dim // W_CHUNKS

    def w_copy(c):
        return pltpu.make_async_copy(wq_ref.at[pl.ds(c * depth, depth)], w_buf.at[c], w_sem.at[c])

    def k_copy(b):
        return pltpu.make_async_copy(k_ref.at[b], k_buf.at[b], k_sem.at[b])

    def v_copy(b):
        return pltpu.make_async_copy(v_ref.at[b], v_buf.at[b], v_sem.at[b])

    def k_back(b):
        return pltpu.make_async_copy(k_buf.at[b], k_out.at[b], ko_sem.at[b])

    def v_back(b):
        return pltpu.make_async_copy(v_buf.at[b], v_out.at[b], vo_sem.at[b])

    for c in range(W_CHUNKS):
        w_copy(c).start()
    for b in range(rows):
        k_copy(b).start()
        v_copy(b).start()

    x = x_ref[...].astype(F32)
    scale = lax.rsqrt(jnp.mean(x * x, axis=-1, keepdims=True) + NORM_EPS)
    r_buf[...] = (x * scale * gain_ref[...]).astype(BF16)
    qkv = None
    for c in range(W_CHUNKS):
        w_copy(c).wait()
        term = jnp.dot(r_buf[:, c * depth:(c + 1) * depth], w_buf[c], preferred_element_type=F32)
        qkv = term if qkv is None else qkv + term

    cos, sin = cos_ref[...], sin_ref[...]

    def rotate(vals):
        out = vals * cos + pltpu.roll(vals, 64, 1) * sin
        return out.astype(BF16).astype(F32)

    for kv in range(2):
        base = kv * 768
        for h in range(4):
            q_buf[:, kv * 4 + h, :] = rotate(qkv[:, base + h * 128:base + (h + 1) * 128])
        kn_buf[kv] = rotate(qkv[:, base + 512:base + 640])
        vn_buf[kv] = qkv[:, base + 640:base + 768].astype(BF16).astype(F32)

    lane = lax.broadcasted_iota(jnp.int32, (8, keys), 1)
    head = lax.broadcasted_iota(jnp.int32, (8, keys), 0)
    own = (lane & 1) == (head >> 2)
    slot = lane >> 1
    row16 = lax.broadcasted_iota(jnp.int32, (16, 128), 0)
    stat_col = lax.broadcasted_iota(jnp.int32, (8, 128), 1)
    stat_row = lax.broadcasted_iota(jnp.int32, (8, 128), 0)

    def put(ref, new_buf, b, ploc):
        start = pl.multiple_of((jnp.clip(ploc * 2, 0, keys - 2) // 16) * 16, 16)
        block = ref[b, pl.ds(start, 16), :].astype(F32)
        first = new_buf[0, pl.ds(b, 1), :]
        second = new_buf[1, pl.ds(b, 1), :]
        at = row16 + start
        block = jnp.where(at == ploc * 2, first, block)
        block = jnp.where(at == ploc * 2 + 1, second, block)
        ref[b, pl.ds(start, 16), :] = block.astype(BF16)

    def group(g, carry):
        m_all, l_all = carry
        ids = [g * GROUP + i for i in range(GROUP)]
        plocs = [ploc_ref[b] for b in ids]
        scores, masks = [], []
        for b, ploc in zip(ids, plocs):
            k_copy(b).wait()
            put(k_buf, kn_buf, b, ploc)
            k_back(b).start()
            s = lax.dot_general(
                q_buf[b].astype(BF16), k_buf[b], (((1,), (1,)), ((), ())), preferred_element_type=F32
            )
            scores.append(s)
        probs, sums = [], []
        for b, ploc, s in zip(ids, plocs, scores):
            mask = own & (slot <= ploc) & (slot >= ploc - WINDOW)
            s = jnp.where(mask, s * (128 ** -0.5), NEG)
            m = jnp.max(s, axis=-1, keepdims=True)
            w = jnp.where(mask, jnp.exp(s - m), 0.0)
            l = jnp.sum(w, axis=-1, keepdims=True)
            at = stat_col == b * 8 + stat_row
            m_all = jnp.where(at, m, m_all)
            l_all = jnp.where(at, l, l_all)
            probs.append(w.astype(BF16))
        for b, ploc, w in zip(ids, plocs, probs):
            v_copy(b).wait()
            put(v_buf, vn_buf, b, ploc)
            v_back(b).start()
            part_ref[b] = jnp.dot(w, v_buf[b], preferred_element_type=F32)
        return m_all, l_all

    zero = jnp.zeros((8, 128), F32)
    m_all, l_all = lax.fori_loop(0, rows // GROUP, group, (zero, zero))
    part_ref[rows] = m_all
    part_ref[rows + 1] = l_all
    for b in range(rows):
        k_back(b).wait()
        v_back(b).wait()


def layer_kernel(
    part_ref, x_ref, gain_ref, wo_ref, wg_ref, wd_ref, out_ref,
    wo_buf, wg_buf, wd_buf, part_rx, o_buf, ob_buf, rs_tx, rs_rx, ag_buf, ss_buf,
    act_buf, rs2_tx, rs2_rx, ag2_buf,
    wo_sem, wg_sem, wd_sem, a_sem, b_sem, s_sem, g_sem, c_sem, d_sem, e_sem,
):
    dp, t, s = lax.axis_index("dp"), lax.axis_index("tp"), lax.axis_index("sp")
    rows = x_ref.shape[0]
    units = wg_buf.shape[1] // 2
    ffn = wd_ref.shape[0]
    me = s * TP + t

    def peer(off):
        return (dp, t ^ off[0], s ^ off[1])

    def piece_of(off):
        return (s ^ off[1]) * TP + (t ^ off[0])

    def remote(src, dst, sems, k, off):
        return pltpu.make_async_remote_copy(
            src_ref=src, dst_ref=dst, send_sem=sems.at[0, k], recv_sem=sems.at[1, k],
            device_id=peer(off), device_id_type=MESH,
        )

    loads_o = []
    for d in range(TP):
        col = pl.multiple_of((s * TP + d) * 256, 256)
        loads_o.append(pltpu.make_async_copy(wo_ref.at[:, pl.ds(col, 256)], wo_buf.at[d], wo_sem.at[d]))
    loads_g = []
    for c in range(8):
        for half in range(2):
            col = pl.multiple_of(half * ffn + s * units, 128)
            loads_g.append(pltpu.make_async_copy(
                wg_ref.at[pl.ds(c * 512, 512), pl.ds(col, units)],
                wg_buf.at[pl.ds(c * 512, 512), pl.ds(half * units, units)],
                wg_sem.at[c, half],
            ))
    loads_d = []
    for c in range(SP):
        col = pl.multiple_of(s * 1024, 1024)
        loads_d.append(pltpu.make_async_copy(
            wd_ref.at[pl.ds(c * units, units), pl.ds(col, 1024)], wd_buf.at[c], wd_sem.at[c]
        ))
    for copy in loads_o + loads_g + loads_d:
        copy.start()

    barrier = pltpu.get_barrier_semaphore()
    for off in OFFSETS:
        pl.semaphore_signal(barrier, inc=1, device_id=peer(off), device_id_type=MESH)
    pl.semaphore_wait(barrier, len(OFFSETS))

    sends = []
    for k in (2, 1, 0):
        copy = remote(part_ref, part_rx.at[k], a_sem, k, (0, k + 1))
        copy.start()
        sends.append(copy)
    for copy in sends:
        copy.wait()
    parts = [part_ref, part_rx.at[0], part_rx.at[1], part_rx.at[2]]
    top = None
    for p in parts:
        top = p[rows] if top is None else jnp.maximum(top, p[rows])
    facs = [jnp.exp(p[rows] - top) for p in parts]
    total = sum(p[rows + 1] * f for p, f in zip(parts, facs))
    inv = 1.0 / total
    facs = [f * inv for f in facs]
    lane8 = lax.broadcasted_iota(jnp.int32, (8, 128), 1)
    sub8 = lax.broadcasted_iota(jnp.int32, (8, 128), 0)
    for b in range(rows):
        at = lane8 == sub8 + b * 8
        o = None
        for p, f in zip(parts, facs):
            col = jnp.sum(jnp.where(at, f, 0.0), axis=-1, keepdims=True)
            o = p[b] * col if o is None else o + p[b] * col
        o_buf[b] = o
    for h in range(8):
        ob_buf[:, h * 128:(h + 1) * 128] = o_buf[:, h, :].astype(BF16)

    def reduce_scatter(make_term, tx, rx, sems):
        sends = []
        for dt in (3, 2, 1):
            tx[dt] = make_term(t ^ dt)
            copy = remote(tx.at[dt], rx.at[dt - 1], sems, dt - 1, (dt, 0))
            copy.start()
            sends.append(copy)
        mine = make_term(t)
        for copy in sends:
            copy.wait()
        return mine + rx[0] + rx[1] + rx[2]

    for copy in loads_o:
        copy.wait()
    o_all = ob_buf[...]

    def out_term(d):
        return jnp.dot(o_all, wo_buf[d], preferred_element_type=F32).astype(BF16).astype(F32)

    my_cols = pl.ds(pl.multiple_of(me * 256, 256), 256)
    mid = x_ref[:, my_cols].astype(F32) + reduce_scatter(out_term, rs_tx, rs_rx, b_sem)
    ag_buf[me] = mid
    lane16 = lax.broadcasted_iota(jnp.int32, (rows, 128), 1)
    sub16 = lax.broadcasted_iota(jnp.int32, (rows, 128), 0)
    diag = lane16 == sub16
    sq = jnp.sum(mid * mid, axis=-1, keepdims=True)
    ss_buf[me] = jnp.sum(jnp.where(diag, sq, 0.0), axis=0, keepdims=True)

    order = tuple(reversed(range(len(OFFSETS))))

    def gather_start(buf, sems):
        sends = []
        for k in order:
            copy = remote(buf.at[me], buf.at[me], sems, k, OFFSETS[k])
            copy.start()
            sends.append(copy)
        return sends

    def gather_wait(buf, sems, k):
        slot = piece_of(OFFSETS[k])
        remote(buf.at[slot], buf.at[slot], sems, k, OFFSETS[k]).wait_recv()
        return slot

    ss_sends = gather_start(ss_buf, s_sem)
    ag_sends = gather_start(ag_buf, g_sem)
    for k in range(len(OFFSETS)):
        gather_wait(ss_buf, s_sem, k)
    tot = jnp.sum(ss_buf[...], axis=0)
    mean_sq = jnp.sum(jnp.where(diag, tot, 0.0), axis=-1, keepdims=True) / (16 * 256)
    rstd = lax.rsqrt(mean_sq + NORM_EPS)
    for copy in loads_g:
        copy.wait()
    hid = None
    for k in range(-1, len(OFFSETS)):
        slot = me if k < 0 else gather_wait(ag_buf, g_sem, k)
        at = pl.ds(pl.multiple_of(slot * 256, 256), 256)
        r2 = (ag_buf[slot] * rstd * gain_ref[:, at]).astype(BF16)
        term = jnp.dot(r2, wg_buf[at, :], preferred_element_type=F32)
        hid = term if hid is None else hid + term
    gate, up = hid[:, :units], hid[:, units:]
    act_buf[s] = (gate * jax.nn.sigmoid(gate) * up).astype(BF16).astype(F32)

    act_sends = []
    for k in (2, 1, 0):
        copy = remote(act_buf.at[s], act_buf.at[s], c_sem, k, (0, k + 1))
        copy.start()
        act_sends.append(copy)
    for copy in loads_d:
        copy.wait()
    down = jnp.dot(act_buf[s].astype(BF16), wd_buf[s], preferred_element_type=F32)
    for k in range(3):
        slot = s ^ (k + 1)
        remote(act_buf.at[slot], act_buf.at[slot], c_sem, k, (0, k + 1)).wait_recv()
        down = down + jnp.dot(act_buf[slot].astype(BF16), wd_buf[slot], preferred_element_type=F32)
    down = down.astype(BF16).astype(F32)
    for d in range(TP):
        rs2_tx[d] = down[:, d * 256:(d + 1) * 256]
    sends = []
    for dt in (3, 2, 1):
        copy = remote(rs2_tx.at[t ^ dt], rs2_rx.at[dt - 1], d_sem, dt - 1, (dt, 0))
        copy.start()
        sends.append(copy)
    for copy in sends:
        copy.wait()
    ag2_buf[me] = mid + (rs2_tx[t] + rs2_rx[0] + rs2_rx[1] + rs2_rx[2])
    ag2_sends = gather_start(ag2_buf, e_sem)
    for k in range(len(OFFSETS)):
        gather_wait(ag2_buf, e_sem, k)
    for i in range(16):
        out_ref[:, i * 256:(i + 1) * 256] = ag2_buf[i].astype(BF16)
    for copy in ss_sends + ag_sends + act_sends + ag2_sends:
        copy.wait_send()


def solution(mesh):
    cache_spec = P("dp", "sp", "tp", None)
    vmem = pl.BlockSpec(memory_space=pltpu.VMEM)
    smem = pl.BlockSpec(memory_space=pltpu.SMEM)
    hbm = pl.BlockSpec(memory_space=pltpu.HBM)

    def local_step(hidden, positions, norm_attn, norm_mlp, w_qkv, w_out, w_gate_up, w_down, k_cache, v_cache):
        rows, block_len, kv_local, head_dim = k_cache.shape
        dim = hidden.shape[1]
        keys = block_len * kv_local
        ploc = positions - lax.axis_index("sp") * block_len
        cos, sin = rope_tables(positions, head_dim)
        flat = (rows, keys, head_dim)
        k_upd, v_upd, part = pl.pallas_call(
            attend_kernel,
            out_shape=(
                jax.ShapeDtypeStruct(flat, BF16),
                jax.ShapeDtypeStruct(flat, BF16),
                pltpu.VMEM((rows + 2, 8, 128), F32),
            ),
            in_specs=[smem, vmem, vmem, vmem, vmem, hbm, hbm, hbm],
            out_specs=(hbm, hbm, vmem),
            scratch_shapes=[
                pltpu.VMEM(flat, BF16),
                pltpu.VMEM(flat, BF16),
                pltpu.VMEM((W_CHUNKS, dim // W_CHUNKS, w_qkv.shape[1]), BF16),
                pltpu.VMEM((rows, dim), BF16),
                pltpu.VMEM((rows, 8, 128), F32),
                pltpu.VMEM((2, rows, 128), F32),
                pltpu.VMEM((2, rows, 128), F32),
                pltpu.SemaphoreType.DMA((W_CHUNKS,)),
                pltpu.SemaphoreType.DMA((rows,)),
                pltpu.SemaphoreType.DMA((rows,)),
                pltpu.SemaphoreType.DMA((rows,)),
                pltpu.SemaphoreType.DMA((rows,)),
            ],
            compiler_params=pltpu.CompilerParams(vmem_limit_bytes=62 * 2 ** 20),
            cost_estimate=pl.CostEstimate(flops=10 ** 9, bytes_accessed=3 * 10 ** 7, transcendentals=10 ** 6),
        )(ploc, hidden, norm_attn.reshape(1, dim), cos, sin, w_qkv, k_cache.reshape(flat), v_cache.reshape(flat))
        units = w_down.shape[0] // SP
        result = pl.pallas_call(
            layer_kernel,
            out_shape=jax.ShapeDtypeStruct((rows, dim), BF16),
            in_specs=[vmem, vmem, vmem, hbm, hbm, hbm],
            out_specs=vmem,
            scratch_shapes=[
                pltpu.VMEM((TP, 1024, 256), BF16),
                pltpu.VMEM((dim, 2 * units), BF16),
                pltpu.VMEM((SP, units, 1024), BF16),
                pltpu.VMEM((3, rows + 2, 8, 128), F32),
                pltpu.VMEM((rows, 8, 128), F32),
                pltpu.VMEM((rows, 1024), BF16),
                pltpu.VMEM((TP, rows, 256), F32),
                pltpu.VMEM((3, rows, 256), F32),
                pltpu.VMEM((16, rows, 256), F32),
                pltpu.VMEM((16, 1, 128), F32),
                pltpu.VMEM((SP, rows, units), F32),
                pltpu.VMEM((TP, rows, 256), F32),
                pltpu.VMEM((3, rows, 256), F32),
                pltpu.VMEM((16, rows, 256), F32),
                pltpu.SemaphoreType.DMA((TP,)),
                pltpu.SemaphoreType.DMA((8, 2)),
                pltpu.SemaphoreType.DMA((SP,)),
                pltpu.SemaphoreType.DMA((2, 3)),
                pltpu.SemaphoreType.DMA((2, 3)),
                pltpu.SemaphoreType.DMA((2, 15)),
                pltpu.SemaphoreType.DMA((2, 15)),
                pltpu.SemaphoreType.DMA((2, 3)),
                pltpu.SemaphoreType.DMA((2, 3)),
                pltpu.SemaphoreType.DMA((2, 15)),
            ],
            compiler_params=pltpu.CompilerParams(
                collective_id=0, has_side_effects=True, vmem_limit_bytes=62 * 2 ** 20
            ),
            cost_estimate=pl.CostEstimate(flops=4 * 10 ** 9, bytes_accessed=3 * 10 ** 7, transcendentals=10 ** 6),
        )(part, hidden, norm_mlp.reshape(1, dim), w_out, w_gate_up, w_down)
        return result, k_upd.reshape(k_cache.shape), v_upd.reshape(v_cache.shape)

    return jax.shard_map(
        local_step, mesh=mesh,
        in_specs=(P("dp", None), P("dp"), P(None), P(None), P(None, "tp"), P("tp", None), P(None, "tp"), P("tp", None), cache_spec, cache_spec),
        out_specs=(P("dp", None), cache_spec, cache_spec), check_vma=False,
    )
```

```python
import jax
import jax.numpy as jnp
import numpy as np
from jax import lax
from jax.experimental import pallas as pl
from jax.experimental.pallas import tpu as pltpu
from jax.sharding import PartitionSpec as P

WINDOW = 2047
ROPE_BASE = 10000.0
NORM_EPS = 1e-5
MESH = pl.DeviceIdType.MESH
F32 = jnp.float32
BF16 = jnp.bfloat16
NEG = float(jnp.finfo(jnp.float32).min)

TP = 4
SP = 4
W_CHUNKS = 8
GROUP = 4
OFFSETS = (
    (0, 1), (0, 3), (0, 2), (1, 1), (1, 0), (1, 3), (1, 2), (2, 1), (2, 0),
    (2, 3), (2, 2), (3, 1), (3, 0), (3, 3), (3, 2),
)
VIA = {off: off if off[1] & 1 else (0, 1) for off in OFFSETS}


def add_offsets(a, b):
    return (a[0] ^ b[0], a[1] ^ b[1])


def attend_kernel(
    pos_ref, freq_ref, x_ref, gain_ref, wq_ref, k_ref, v_ref,
    k_out, v_out, part_ref,
    pos, freq, x_buf, gain, k_buf, v_buf, w_buf, r_buf, q_buf, kn_buf, vn_buf,
    in_sem, w_sem, k_sem, v_sem, ko_sem, vo_sem,
):
    rows, dim = x_ref.shape
    keys = k_ref.shape[1]
    depth = dim // W_CHUNKS

    def w_copy(c):
        return pltpu.make_async_copy(wq_ref.at[pl.ds(c * depth, depth)], w_buf.at[c], w_sem.at[c])

    def k_copy(b):
        return pltpu.make_async_copy(k_ref.at[b], k_buf.at[b], k_sem.at[b])

    def v_copy(b):
        return pltpu.make_async_copy(v_ref.at[b], v_buf.at[b], v_sem.at[b])

    def k_back(b):
        return pltpu.make_async_copy(k_buf.at[b], k_out.at[b], ko_sem.at[b])

    def v_back(b):
        return pltpu.make_async_copy(v_buf.at[b], v_out.at[b], vo_sem.at[b])

    small = [
        pltpu.make_async_copy(src, dst, in_sem.at[i])
        for i, (src, dst) in enumerate(((x_ref, x_buf), (gain_ref, gain), (freq_ref, freq), (pos_ref, pos)))
    ]
    for copy in small:
        copy.start()
    for c in range(W_CHUNKS):
        w_copy(c).start()
    small[0].wait()
    small[1].wait()
    x = x_buf[...].astype(F32)
    scale = lax.rsqrt(jnp.mean(x * x, axis=-1, keepdims=True) + NORM_EPS)
    r_buf[...] = (x * scale * gain[...]).astype(BF16)
    small[2].wait()
    small[3].wait()
    row_id = lax.broadcasted_iota(jnp.int32, (rows, 128), 0)
    lane_id = lax.broadcasted_iota(jnp.int32, (rows, 128), 1)
    pos_col = jnp.zeros((rows, 128), jnp.int32)
    for b in range(rows):
        pos_col = jnp.where(row_id == b, pos[b], pos_col)
    angle = pos_col.astype(F32) * freq[...]
    cos = jnp.cos(angle)
    sin = jnp.where(lane_id < 64, -jnp.sin(angle), jnp.sin(angle))

    per = rows // W_CHUNKS
    qkv = None
    for c in range(W_CHUNKS):
        w_copy(c).wait()
        for b in range(c * per, (c + 1) * per):
            k_copy(b).start()
            v_copy(b).start()
        term = jnp.dot(r_buf[:, c * depth:(c + 1) * depth], w_buf[c], preferred_element_type=F32)
        qkv = term if qkv is None else qkv + term

    def rotate(vals):
        out = vals * cos + pltpu.roll(vals, 64, 1) * sin
        return out.astype(BF16).astype(F32)

    for kv in range(2):
        base = kv * 768
        for h in range(4):
            q_buf[:, kv * 4 + h, :] = rotate(qkv[:, base + h * 128:base + (h + 1) * 128])
        kn_buf[kv] = rotate(qkv[:, base + 512:base + 640])
        vn_buf[kv] = qkv[:, base + 640:base + 768].astype(BF16).astype(F32)

    first_slot = lax.axis_index("sp") * (keys // 2)
    lane = lax.broadcasted_iota(jnp.int32, (8, keys), 1)
    head = lax.broadcasted_iota(jnp.int32, (8, keys), 0)
    own = (lane & 1) == (head >> 2)
    slot = lane >> 1
    row16 = lax.broadcasted_iota(jnp.int32, (16, 128), 0)
    stat_col = lax.broadcasted_iota(jnp.int32, (8, 128), 1)
    stat_row = lax.broadcasted_iota(jnp.int32, (8, 128), 0)

    def put(ref, new_buf, b, ploc):
        start = pl.multiple_of((jnp.clip(ploc * 2, 0, keys - 2) // 16) * 16, 16)
        block = ref[b, pl.ds(start, 16), :].astype(F32)
        first = new_buf[0, pl.ds(b, 1), :]
        second = new_buf[1, pl.ds(b, 1), :]
        at = row16 + start
        block = jnp.where(at == ploc * 2, first, block)
        block = jnp.where(at == ploc * 2 + 1, second, block)
        ref[b, pl.ds(start, 16), :] = block.astype(BF16)

    def stage(b):
        ploc = pos[b] - first_slot
        k_copy(b).wait()
        put(k_buf, kn_buf, b, ploc)
        k_back(b).start()
        v_copy(b).wait()
        put(v_buf, vn_buf, b, ploc)
        v_back(b).start()

    def compute(g, carry):
        m_all, l_all = carry
        ids = [g * GROUP + i for i in range(GROUP)]
        plocs = [pos[b] - first_slot for b in ids]
        scores = [
            lax.dot_general(
                q_buf[b].astype(BF16), k_buf[b], (((1,), (1,)), ((), ())), preferred_element_type=F32
            )
            for b in ids
        ]
        probs = []
        for b, ploc, s in zip(ids, plocs, scores):
            mask = own & (slot <= ploc) & (slot >= ploc - WINDOW)
            s = jnp.where(mask, s * (128 ** -0.5), NEG)
            m = jnp.max(s, axis=-1, keepdims=True)
            w = jnp.where(mask, jnp.exp(s - m), 0.0)
            l = jnp.sum(w, axis=-1, keepdims=True)
            at = stat_col == b * 8 + stat_row
            m_all = jnp.where(at, m, m_all)
            l_all = jnp.where(at, l, l_all)
            probs.append(w.astype(BF16))
        for b, w in zip(ids, probs):
            part_ref[b] = jnp.dot(w, v_buf[b], preferred_element_type=F32)
        return m_all, l_all

    def group(g, carry):
        for i in range(GROUP):
            stage((g + 1) * GROUP + i)
        return compute(g, carry)

    for b in range(GROUP):
        stage(b)
    zero = jnp.zeros((8, 128), F32)
    last = rows // GROUP - 1
    carry = lax.fori_loop(0, last, group, (zero, zero))
    m_all, l_all = compute(last, carry)
    part_ref[rows] = m_all
    part_ref[rows + 1] = l_all
    for b in range(rows):
        k_back(b).wait()
        v_back(b).wait()


def layer_kernel(
    part_ref, x_ref, gain_ref, wo_ref, wg_ref, wd_ref, out_ref,
    x_buf, gain, wo_buf, wg_buf, wd_buf, part_rx, o_buf, ob_buf, rs_tx, rs_rx, ag_buf, ss_buf,
    act_buf, dn_buf, rs2_tx, rs2_rx, ag2_buf,
    in_sem, wo_sem, wg_sem, wd_sem, a_sem, b_sem, s_sem, g_sem, c_sem, d_sem, e_sem,
):
    dp, t, s = lax.axis_index("dp"), lax.axis_index("tp"), lax.axis_index("sp")
    rows = x_ref.shape[0]
    units = wg_buf.shape[1] // 2
    ffn = wd_ref.shape[0]

    def peer(off):
        return (dp, t ^ off[0], s ^ off[1])

    def piece_of(off):
        return (s ^ off[1] ^ 1) * TP + (t ^ off[0])

    me = piece_of((0, 0))

    def remote(src, dst, sems, k, off):
        return pltpu.make_async_remote_copy(
            src_ref=src, dst_ref=dst, send_sem=sems.at[0, k], recv_sem=sems.at[1, k],
            device_id=peer(off), device_id_type=MESH,
        )

    loads_in = [
        pltpu.make_async_copy(x_ref, x_buf, in_sem.at[0]),
        pltpu.make_async_copy(gain_ref, gain, in_sem.at[1]),
    ]
    loads_o = []
    for d in range(TP):
        col = pl.multiple_of((s * TP + d) * 256, 256)
        loads_o.append(pltpu.make_async_copy(wo_ref.at[:, pl.ds(col, 256)], wo_buf.at[d], wo_sem.at[d]))
    loads_g = []
    for c in range(8):
        for half in range(2):
            col = pl.multiple_of(half * ffn + s * units, 128)
            loads_g.append(pltpu.make_async_copy(
                wg_ref.at[pl.ds(c * 512, 512), pl.ds(col, units)],
                wg_buf.at[pl.ds(c * 512, 512), pl.ds(half * units, units)],
                wg_sem.at[c, half],
            ))
    loads_d = []
    for c in range(SP):
        col = pl.multiple_of(s * 1024, 1024)
        loads_d.append(pltpu.make_async_copy(
            wd_ref.at[pl.ds(c * units, units), pl.ds(col, 1024)], wd_buf.at[c], wd_sem.at[c]
        ))
    barrier = pltpu.get_barrier_semaphore()
    for off in OFFSETS:
        pl.semaphore_signal(barrier, inc=1, device_id=peer(off), device_id_type=MESH)
    for copy in loads_in + loads_o + loads_g + loads_d:
        copy.start()
    pl.semaphore_wait(barrier, len(OFFSETS))

    a_sends = []
    for k, off in ((2, (0, 3)), (0, (0, 1))):
        copy = remote(part_ref, part_rx.at[k], a_sem, k, off)
        copy.start()
        a_sends.append(copy)
    remote(part_ref, part_rx.at[2], a_sem, 2, (0, 3)).wait_recv()
    copy = remote(part_rx.at[2], part_rx.at[1], a_sem, 1, (0, 1))
    copy.start()
    a_sends.append(copy)
    for k in range(2):
        remote(part_ref, part_rx.at[k], a_sem, k, (0, 1)).wait_recv()
    parts = [part_ref, part_rx.at[0], part_rx.at[1], part_rx.at[2]]
    top = None
    for p in parts:
        top = p[rows] if top is None else jnp.maximum(top, p[rows])
    facs = [jnp.exp(p[rows] - top) for p in parts]
    total = sum(p[rows + 1] * f for p, f in zip(parts, facs))
    inv = 1.0 / total
    facs = [f * inv for f in facs]
    lane8 = lax.broadcasted_iota(jnp.int32, (8, 128), 1)
    sub8 = lax.broadcasted_iota(jnp.int32, (8, 128), 0)
    for b in range(rows):
        at = lane8 == sub8 + b * 8
        o = None
        for p, f in zip(parts, facs):
            col = jnp.sum(jnp.where(at, f, 0.0), axis=-1, keepdims=True)
            o = p[b] * col if o is None else o + p[b] * col
        o_buf[b] = o
    for h in range(8):
        ob_buf[:, h * 128:(h + 1) * 128] = o_buf[:, h, :].astype(BF16)

    def reduce_scatter(make_term, tx, rx, sems):
        sends = []
        for dt in (3, 2, 1, 0):
            tx[dt] = make_term(t ^ dt)
            copy = remote(tx.at[dt], rx.at[dt], sems, dt, (dt, 1))
            copy.start()
            sends.append(copy)
        for copy in sends:
            copy.wait()
        return rx[0] + rx[1] + rx[2] + rx[3]

    for copy in loads_in + loads_o:
        copy.wait()
    o_all = ob_buf[...]

    def out_term(d):
        return jnp.dot(o_all, wo_buf[d], preferred_element_type=F32).astype(BF16).astype(F32)

    my_cols = pl.ds(pl.multiple_of(me * 256, 256), 256)
    mid = x_buf[:, my_cols].astype(F32) + reduce_scatter(out_term, rs_tx, rs_rx, b_sem)
    ag_buf[me] = mid
    lane16 = lax.broadcasted_iota(jnp.int32, (rows, 128), 1)
    sub16 = lax.broadcasted_iota(jnp.int32, (rows, 128), 0)
    diag = lane16 == sub16
    sq = jnp.sum(mid * mid, axis=-1, keepdims=True)
    ss_buf[me] = jnp.sum(jnp.where(diag, sq, 0.0), axis=0, keepdims=True)

    def broadcast(buf, sems):
        sends = []
        for k in reversed(range(len(OFFSETS))):
            copy = remote(buf.at[me], buf.at[me], sems, k, OFFSETS[k])
            copy.start()
            sends.append(copy)
        return sends

    class Gather:
        def __init__(self, buf, sems):
            self.buf, self.sems, self.sends = buf, sems, []

        def send(self, have):
            for k in reversed(range(len(OFFSETS))):
                off = OFFSETS[k]
                if add_offsets(off, VIA[off]) == have:
                    slot = piece_of(have)
                    copy = remote(self.buf.at[slot], self.buf.at[slot], self.sems, k, VIA[off])
                    copy.start()
                    self.sends.append(copy)

        def wait(self, k, forward=True):
            off = OFFSETS[k]
            slot = piece_of(off)
            remote(self.buf.at[slot], self.buf.at[slot], self.sems, k, VIA[off]).wait_recv()
            if forward:
                self.send(off)
            return slot

    ss_sends = broadcast(ss_buf, s_sem)
    gather = Gather(ag_buf, g_sem)
    gather.send((0, 0))
    for k in range(len(OFFSETS)):
        slot = piece_of(OFFSETS[k])
        remote(ss_buf.at[slot], ss_buf.at[slot], s_sem, k, OFFSETS[k]).wait_recv()
    tot = jnp.sum(ss_buf[...], axis=0)
    mean_sq = jnp.sum(jnp.where(diag, tot, 0.0), axis=-1, keepdims=True) / (16 * 256)
    rstd = lax.rsqrt(mean_sq + NORM_EPS)
    for copy in loads_g:
        copy.wait()
    hid = None
    for k in range(-1, len(OFFSETS)):
        slot = me if k < 0 else gather.wait(k)
        at = pl.ds(pl.multiple_of(slot * 256, 256), 256)
        r2 = (ag_buf[slot] * rstd * gain[:, at]).astype(BF16)
        term = jnp.dot(r2, wg_buf[at, :], preferred_element_type=F32)
        hid = term if hid is None else hid + term
    gate, up = hid[:, :units], hid[:, units:]
    act_buf[s] = (gate * jax.nn.sigmoid(gate) * up).astype(BF16).astype(F32)

    act_sends = []

    def act_send(slot, k, off):
        copy = remote(act_buf.at[slot], act_buf.at[slot], c_sem, k, off)
        copy.start()
        act_sends.append(copy)

    act_send(s, 2, (0, 3))
    act_send(s, 0, (0, 1))
    for copy in loads_d:
        copy.wait()
    down = jnp.dot(act_buf[s].astype(BF16), wd_buf[s], preferred_element_type=F32)
    for k in (0, 2, 1):
        slot = s ^ (k + 1)
        remote(act_buf.at[slot], act_buf.at[slot], c_sem, k, (0, 1)).wait_recv()
        if k == 2:
            act_send(slot, 1, (0, 1))
        down = down + jnp.dot(act_buf[slot].astype(BF16), wd_buf[slot], preferred_element_type=F32)
    rs2_buf = down.astype(BF16).astype(F32)
    for d in range(TP):
        dn_buf[d] = rs2_buf[:, d * 256:(d + 1) * 256]

    def down_term(d):
        return dn_buf[d]

    final = mid + reduce_scatter(down_term, rs2_tx, rs2_rx, d_sem)
    gather2 = Gather(ag2_buf, e_sem)
    gather2.buf[me] = final
    gather2.send((0, 0))
    for k in range(len(OFFSETS)):
        gather2.wait(k)
    for i in range(16):
        out_ref[:, i * 256:(i + 1) * 256] = gather2.buf[i]
    for copy in a_sends + ss_sends + gather.sends + act_sends + gather2.sends:
        copy.wait_send()


def solution(mesh):
    cache_spec = P("dp", "sp", "tp", None)
    vmem = pl.BlockSpec(memory_space=pltpu.VMEM)
    hbm = pl.BlockSpec(memory_space=pltpu.HBM)

    def in_hbm(*arrays):
        return tuple(pltpu.with_memory_space_constraint(a, pltpu.HBM) for a in arrays)

    def local_step(hidden, positions, norm_attn, norm_mlp, w_qkv, w_out, w_gate_up, w_down, k_cache, v_cache):
        rows, block_len, kv_local, head_dim = k_cache.shape
        dim = hidden.shape[1]
        flat = (rows, block_len * kv_local, head_dim)
        freq = ROPE_BASE ** (-np.arange(0, head_dim, 2, dtype=np.float64) / head_dim)
        freq = jnp.asarray(np.concatenate([freq, freq])[None].astype(np.float32))
        k_upd, v_upd, part = pl.pallas_call(
            attend_kernel,
            out_shape=(
                jax.ShapeDtypeStruct(flat, BF16),
                jax.ShapeDtypeStruct(flat, BF16),
                pltpu.VMEM((rows + 2, 8, 128), F32),
            ),
            in_specs=[hbm] * 7,
            out_specs=(hbm, hbm, vmem),
            scratch_shapes=[
                pltpu.SMEM((rows,), jnp.int32),
                pltpu.VMEM((1, head_dim), F32),
                pltpu.VMEM((rows, dim), BF16),
                pltpu.VMEM((1, dim), F32),
                pltpu.VMEM(flat, BF16),
                pltpu.VMEM(flat, BF16),
                pltpu.VMEM((W_CHUNKS, dim // W_CHUNKS, w_qkv.shape[1]), BF16),
                pltpu.VMEM((rows, dim), BF16),
                pltpu.VMEM((rows, 8, 128), F32),
                pltpu.VMEM((2, rows, 128), F32),
                pltpu.VMEM((2, rows, 128), F32),
                pltpu.SemaphoreType.DMA((4,)),
                pltpu.SemaphoreType.DMA((W_CHUNKS,)),
                pltpu.SemaphoreType.DMA((rows,)),
                pltpu.SemaphoreType.DMA((rows,)),
                pltpu.SemaphoreType.DMA((rows,)),
                pltpu.SemaphoreType.DMA((rows,)),
            ],
            compiler_params=pltpu.CompilerParams(vmem_limit_bytes=36 * 2 ** 20),
            cost_estimate=pl.CostEstimate(flops=10 ** 9, bytes_accessed=3 * 10 ** 7, transcendentals=10 ** 6),
        )(*in_hbm(
            positions, freq, hidden, norm_attn.reshape(1, dim), w_qkv, k_cache.reshape(flat), v_cache.reshape(flat)
        ))
        units = w_down.shape[0] // SP
        result = pl.pallas_call(
            layer_kernel,
            out_shape=pltpu.VMEM((rows, dim), F32),
            in_specs=[vmem] + [hbm] * 5,
            out_specs=vmem,
            scratch_shapes=[
                pltpu.VMEM((rows, dim), BF16),
                pltpu.VMEM((1, dim), F32),
                pltpu.VMEM((TP, 1024, 256), BF16),
                pltpu.VMEM((dim, 2 * units), BF16),
                pltpu.VMEM((SP, units, 1024), BF16),
                pltpu.VMEM((3, rows + 2, 8, 128), F32),
                pltpu.VMEM((rows, 8, 128), F32),
                pltpu.VMEM((rows, 1024), BF16),
                pltpu.VMEM((TP, rows, 256), F32),
                pltpu.VMEM((TP, rows, 256), F32),
                pltpu.VMEM((16, rows, 256), F32),
                pltpu.VMEM((16, 1, 128), F32),
                pltpu.VMEM((SP, rows, units), F32),
                pltpu.VMEM((TP, rows, 256), F32),
                pltpu.VMEM((TP, rows, 256), F32),
                pltpu.VMEM((TP, rows, 256), F32),
                pltpu.VMEM((16, rows, 256), F32),
                pltpu.SemaphoreType.DMA((2,)),
                pltpu.SemaphoreType.DMA((TP,)),
                pltpu.SemaphoreType.DMA((8, 2)),
                pltpu.SemaphoreType.DMA((SP,)),
                pltpu.SemaphoreType.DMA((2, 3)),
                pltpu.SemaphoreType.DMA((2, 4)),
                pltpu.SemaphoreType.DMA((2, 15)),
                pltpu.SemaphoreType.DMA((2, 15)),
                pltpu.SemaphoreType.DMA((2, 3)),
                pltpu.SemaphoreType.DMA((2, 4)),
                pltpu.SemaphoreType.DMA((2, 15)),
            ],
            compiler_params=pltpu.CompilerParams(
                collective_id=0, has_side_effects=True, vmem_limit_bytes=32 * 2 ** 20
            ),
            cost_estimate=pl.CostEstimate(flops=4 * 10 ** 9, bytes_accessed=3 * 10 ** 7, transcendentals=10 ** 6),
        )(part, *in_hbm(hidden, norm_mlp.reshape(1, dim), w_out, w_gate_up, w_down))
        return result.astype(BF16), k_upd.reshape(k_cache.shape), v_upd.reshape(v_cache.shape)

    return jax.shard_map(
        local_step, mesh=mesh,
        in_specs=(P("dp", None), P("dp"), P(None), P(None), P(None, "tp"), P("tp", None), P(None, "tp"), P("tp", None), cache_spec, cache_spec),
        out_specs=(P("dp", None), cache_spec, cache_spec), check_vma=False,
    )
```

```python
import jax
import jax.numpy as jnp
import numpy as np
from jax import lax
from jax.experimental import pallas as pl
from jax.experimental.pallas import tpu as pltpu
from jax.sharding import PartitionSpec as P

WINDOW = 2047
ROPE_BASE = 10000.0
NORM_EPS = 1e-5
MESH = pl.DeviceIdType.MESH
F32 = jnp.float32
BF16 = jnp.bfloat16
NEG = float(jnp.finfo(jnp.float32).min)

TP = 4
SP = 4
W_CHUNKS = 8
GROUP = 4
AHEAD = 4
OFFSETS = (
    (0, 1), (0, 3), (1, 1), (2, 1), (1, 3), (3, 1), (2, 3), (3, 3),
    (0, 2), (1, 0), (2, 0), (1, 2), (3, 0), (2, 2), (3, 2),
)
VIA = {off: off if off[1] & 1 else (0, 1) for off in OFFSETS}


def add_offsets(a, b):
    return (a[0] ^ b[0], a[1] ^ b[1])


def layer_kernel(
    pos_ref, freq_ref, x_ref, gain_ref, gain2_ref, wq_ref, k_ref, v_ref, wo_ref, wg_ref, wd_ref,
    out_ref, k_buf, v_buf, kn_buf, vn_buf,
    pos, freq, x_buf, gain, gain2, wq_buf, wo_buf, wg_buf, wd_buf,
    r_buf, q_buf, part, part_rx, o_buf, ob_buf, rs_tx, rs_rx, ag_buf, ss_buf, r2_buf,
    act_buf, dn_buf, rs2_tx, rs2_rx, ag2_buf,
    in_sem, wq_sem, k_sem, v_sem, wo_sem, wg_sem, wd_sem,
    a_sem, b_sem, s_sem, g_sem, c_sem, d_sem, e_sem,
):
    dp, t, s = lax.axis_index("dp"), lax.axis_index("tp"), lax.axis_index("sp")
    rows, dim = x_ref.shape
    keys = k_ref.shape[1]
    units = wg_buf.shape[1] // 2
    ffn = wd_ref.shape[0]
    depth = dim // W_CHUNKS

    def peer(off):
        return (dp, t ^ off[0], s ^ off[1])

    def piece_of(off):
        return (s ^ off[1] ^ 1) * TP + (t ^ off[0])

    me = piece_of((0, 0))

    def remote(src, dst, sems, k, off):
        return pltpu.make_async_remote_copy(
            src_ref=src, dst_ref=dst, send_sem=sems.at[0, k], recv_sem=sems.at[1, k],
            device_id=peer(off), device_id_type=MESH,
        )

    small = [
        pltpu.make_async_copy(src, dst, in_sem.at[i])
        for i, (src, dst) in enumerate((
            (x_ref, x_buf), (gain_ref, gain), (freq_ref, freq), (pos_ref, pos), (gain2_ref, gain2)
        ))
    ]
    for copy in small:
        copy.start()

    def wq_copy(c):
        return pltpu.make_async_copy(wq_ref.at[pl.ds(c * depth, depth)], wq_buf.at[c], wq_sem.at[c])

    def k_copy(b):
        return pltpu.make_async_copy(k_ref.at[b], k_buf.at[b], k_sem.at[b])

    def v_copy(b):
        return pltpu.make_async_copy(v_ref.at[b], v_buf.at[b], v_sem.at[b])

    def wo_copy(d):
        col = pl.multiple_of((s * TP + d) * 256, 256)
        return pltpu.make_async_copy(wo_ref.at[:, pl.ds(col, 256)], wo_buf.at[d], wo_sem.at[d])

    def wg_copy(c, half):
        col = pl.multiple_of(half * ffn + s * units, 128)
        return pltpu.make_async_copy(
            wg_ref.at[pl.ds(c * 512, 512), pl.ds(col, units)],
            wg_buf.at[pl.ds(c * 512, 512), pl.ds(half * units, units)],
            wg_sem.at[c, half],
        )

    def wd_copy(c):
        col = pl.multiple_of(s * 1024, 1024)
        return pltpu.make_async_copy(
            wd_ref.at[pl.ds(c * units, units), pl.ds(col, 1024)], wd_buf.at[c], wd_sem.at[c]
        )

    def start_kv(b):
        k_copy(b).start()
        v_copy(b).start()

    for c in range(W_CHUNKS):
        wq_copy(c).start()
    for b in range(AHEAD):
        start_kv(b)
    barrier = pltpu.get_barrier_semaphore()
    for off in OFFSETS:
        pl.semaphore_signal(barrier, inc=1, device_id=peer(off), device_id_type=MESH)

    small[0].wait()
    small[1].wait()
    x = x_buf[...].astype(F32)
    scale = lax.rsqrt(jnp.mean(x * x, axis=-1, keepdims=True) + NORM_EPS)
    r_buf[...] = (x * scale * gain[...]).astype(BF16)
    small[2].wait()
    small[3].wait()
    row_id = lax.broadcasted_iota(jnp.int32, (rows, 128), 0)
    lane_id = lax.broadcasted_iota(jnp.int32, (rows, 128), 1)
    diag = row_id == lane_id

    qkv = None
    for c in range(W_CHUNKS):
        wq_copy(c).wait()
        for b in range(AHEAD + c, rows if c == W_CHUNKS - 1 else AHEAD + c + 1):
            start_kv(b)
        term = jnp.dot(r_buf[:, c * depth:(c + 1) * depth], wq_buf[c], preferred_element_type=F32)
        qkv = term if qkv is None else qkv + term
        if c == 1:
            pos_col = jnp.zeros((rows, 128), jnp.int32)
            for b in range(rows):
                pos_col = jnp.where(row_id == b, pos[b], pos_col)
            angle = pos_col.astype(F32) * freq[...]
            cos = jnp.cos(angle)
            sin = jnp.sin(angle)
            sin = jnp.where(lane_id < 64, -sin, sin)

    def rotate(vals):
        out = vals * cos + pltpu.roll(vals, 64, 1) * sin
        return out.astype(BF16).astype(F32)

    for kv in range(2):
        base = kv * 768
        for h in range(4):
            q_buf[:, kv * 4 + h, :] = rotate(qkv[:, base + h * 128:base + (h + 1) * 128])
        kn_buf[kv] = rotate(qkv[:, base + 512:base + 640])
        vn_buf[kv] = qkv[:, base + 640:base + 768].astype(BF16).astype(F32)

    pl.semaphore_wait(barrier, len(OFFSETS))
    first_slot = s * (keys // 2)
    lane = lax.broadcasted_iota(jnp.int32, (8, keys), 1)
    head = lax.broadcasted_iota(jnp.int32, (8, keys), 0)
    own = (lane & 1) == (head >> 2)
    slot_id = lane >> 1
    lane8 = lax.broadcasted_iota(jnp.int32, (8, 128), 1)
    sub8 = lax.broadcasted_iota(jnp.int32, (8, 128), 0)
    low_heads = sub8 < 4
    scale = 128 ** -0.5

    def new_rows(buf, b):
        return jnp.where(low_heads, buf[0, pl.ds(b, 1), :], buf[1, pl.ds(b, 1), :])

    def a_rows(g):
        return pl.ds(g * GROUP, GROUP + (2 if g == rows // GROUP - 1 else 0))

    def a_copy(g, k, off):
        return remote(part.at[a_rows(g)], part_rx.at[k, a_rows(g)], a_sem.at[g], k, off)

    def a_forward(g):
        return remote(part_rx.at[2, a_rows(g)], part_rx.at[1, a_rows(g)], a_sem.at[g], 1, (0, 1))

    a_sends = []
    m_all = jnp.zeros((8, 128), F32)
    l_all = jnp.zeros((8, 128), F32)
    n_all = jnp.zeros((8, 128), F32)
    for g in range(rows // GROUP):
        ids = range(g * GROUP, (g + 1) * GROUP)
        scores = []
        for b in ids:
            k_copy(b).wait()
            q = q_buf[b]
            scores.append(lax.dot_general(
                q.astype(BF16), k_buf[b], (((1,), (1,)), ((), ())), preferred_element_type=F32
            ))
            fresh = jnp.sum(q * new_rows(kn_buf, b), axis=-1, keepdims=True) * scale
            n_all = jnp.where(lane8 == sub8 + b * 8, fresh, n_all)
        probs = []
        for b, sc in zip(ids, scores):
            ploc = pos[b] - first_slot
            mask = own & (slot_id < ploc) & (slot_id >= ploc - WINDOW)
            sc = jnp.where(mask, sc * scale, NEG)
            m = jnp.max(sc, axis=-1, keepdims=True)
            w = jnp.where(mask, jnp.exp(sc - m), 0.0)
            l = jnp.sum(w, axis=-1, keepdims=True)
            at = lane8 == sub8 + b * 8
            m_all = jnp.where(at, m, m_all)
            l_all = jnp.where(at, l, l_all)
            probs.append(w.astype(BF16))
        for b, w in zip(ids, probs):
            v_copy(b).wait()
            part[b] = jnp.dot(w, v_buf[b], preferred_element_type=F32)
        if g == rows // GROUP - 1:
            part[rows] = m_all
            part[rows + 1] = l_all
        for k, off in ((2, (0, 3)), (0, (0, 1))):
            copy = a_copy(g, k, off)
            copy.start()
            a_sends.append(copy)
        if g == 1:
            for d in range(TP):
                wo_copy(d).start()
        if g >= 2:
            for c in range((g - 2) * 4, (g - 1) * 4):
                wg_copy(c, 0).start()
                wg_copy(c, 1).start()
    for c in range(SP):
        wd_copy(c).start()

    for g in range(rows // GROUP):
        a_copy(g, 2, (0, 3)).wait_recv()
        copy = a_forward(g)
        copy.start()
        a_sends.append(copy)
    for g in range(rows // GROUP):
        a_copy(g, 0, (0, 1)).wait_recv()
        a_copy(g, 1, (0, 1)).wait_recv()
    parts = [part, part_rx.at[0], part_rx.at[1], part_rx.at[2]]
    top = n_all
    for p in parts:
        top = jnp.maximum(top, p[rows])
    facs = [jnp.exp(p[rows] - top) for p in parts]
    fresh = jnp.exp(n_all - top)
    total = fresh
    for p, f in zip(parts, facs):
        total = total + p[rows + 1] * f
    inv = 1.0 / total
    facs = [f * inv for f in facs]
    fresh = fresh * inv
    for b in range(rows):
        at = lane8 == sub8 + b * 8
        o = new_rows(vn_buf, b) * jnp.sum(jnp.where(at, fresh, 0.0), axis=-1, keepdims=True)
        for p, f in zip(parts, facs):
            o = o + p[b] * jnp.sum(jnp.where(at, f, 0.0), axis=-1, keepdims=True)
        o_buf[b] = o
    for h in range(8):
        ob_buf[:, h * 128:(h + 1) * 128] = o_buf[:, h, :].astype(BF16)

    def reduce_scatter(make_term, tx, rx, sems):
        sends = []
        for dt in (3, 2, 1, 0):
            tx[dt] = make_term(t ^ dt)
            copy = remote(tx.at[dt], rx.at[dt], sems, dt, (dt, 1))
            copy.start()
            sends.append(copy)
        for copy in sends:
            copy.wait()
        return rx[0] + rx[1] + rx[2] + rx[3]

    small[4].wait()
    for d in range(TP):
        wo_copy(d).wait()
    o_all = ob_buf[...]

    def out_term(d):
        return jnp.dot(o_all, wo_buf[d], preferred_element_type=F32).astype(BF16).astype(F32)

    my_cols = pl.ds(pl.multiple_of(me * 256, 256), 256)
    mid = x_buf[:, my_cols].astype(F32) + reduce_scatter(out_term, rs_tx, rs_rx, b_sem)
    ag_buf[me] = mid
    sq = jnp.sum(mid * mid, axis=-1, keepdims=True)
    ss_buf[me] = jnp.sum(jnp.where(diag, sq, 0.0), axis=0, keepdims=True)

    class Gather:
        def __init__(self, buf, sems):
            self.buf, self.sems, self.sends = buf, sems, []

        def send(self, have):
            for k in reversed(range(len(OFFSETS))):
                off = OFFSETS[k]
                if add_offsets(off, VIA[off]) == have:
                    slot = piece_of(have)
                    copy = remote(self.buf.at[slot], self.buf.at[slot], self.sems, k, VIA[off])
                    copy.start()
                    self.sends.append(copy)

        def wait(self, off):
            slot = piece_of(off)
            k = OFFSETS.index(off)
            remote(self.buf.at[slot], self.buf.at[slot], self.sems, k, VIA[off]).wait_recv()
            self.send(off)

    ss_sends = []
    for k in sorted(range(len(OFFSETS)), key=lambda i: -OFFSETS[i][0]):
        copy = remote(ss_buf.at[me], ss_buf.at[me], s_sem, k, OFFSETS[k])
        copy.start()
        ss_sends.append(copy)
    gather = Gather(ag_buf, g_sem)
    gather.send((0, 0))
    for off in OFFSETS[:6]:
        gather.wait(off)
    for k in range(len(OFFSETS)):
        slot = piece_of(OFFSETS[k])
        remote(ss_buf.at[slot], ss_buf.at[slot], s_sem, k, OFFSETS[k]).wait_recv()
    tot = jnp.sum(ss_buf[...], axis=0)
    mean_sq = jnp.sum(jnp.where(diag, tot, 0.0), axis=-1, keepdims=True) / dim
    rstd = lax.rsqrt(mean_sq + NORM_EPS)
    for c in range(8):
        wg_copy(c, 0).wait()
        wg_copy(c, 1).wait()

    def gate_up(ds):
        block = s ^ ds ^ 1
        for j in range(TP):
            at = pl.ds(pl.multiple_of((block * TP + j) * 256, 256), 256)
            r2_buf[ds, :, j * 256:(j + 1) * 256] = (ag_buf[block * TP + j] * rstd * gain2[:, at]).astype(BF16)
        at = pl.ds(pl.multiple_of(block * 1024, 1024), 1024)
        return jnp.dot(r2_buf[ds], wg_buf[at, :], preferred_element_type=F32)

    hid = gate_up(1)
    for off in OFFSETS[6:8] + OFFSETS[8:9]:
        gather.wait(off)
    for off in ((1, 0), (2, 0), (3, 0)):
        gather.wait(off)
    hid = hid + gate_up(0) + gate_up(3)
    for off in ((1, 2), (2, 2), (3, 2)):
        gather.wait(off)
    hid = hid + gate_up(2)
    gate, up = hid[:, :units], hid[:, units:]
    act_buf[s] = (gate * jax.nn.sigmoid(gate) * up).astype(BF16).astype(F32)

    act_sends = []

    def act_send(slot, k, off):
        copy = remote(act_buf.at[slot], act_buf.at[slot], c_sem, k, off)
        copy.start()
        act_sends.append(copy)

    act_send(s, 2, (0, 3))
    act_send(s, 0, (0, 1))
    for c in range(SP):
        wd_copy(c).wait()
    down = jnp.dot(act_buf[s].astype(BF16), wd_buf[s], preferred_element_type=F32)
    for k in (0, 2, 1):
        slot = s ^ (k + 1)
        remote(act_buf.at[slot], act_buf.at[slot], c_sem, k, (0, 1)).wait_recv()
        if k == 2:
            act_send(slot, 1, (0, 1))
        down = down + jnp.dot(act_buf[slot].astype(BF16), wd_buf[slot], preferred_element_type=F32)
    down = down.astype(BF16).astype(F32)
    for d in range(TP):
        dn_buf[d] = down[:, d * 256:(d + 1) * 256]

    def down_term(d):
        return dn_buf[d]

    ag2_buf[me] = mid + reduce_scatter(down_term, rs2_tx, rs2_rx, d_sem)
    gather2 = Gather(ag2_buf, e_sem)
    gather2.send((0, 0))
    for off in OFFSETS:
        gather2.wait(off)
    for i in range(16):
        out_ref[:, i * 256:(i + 1) * 256] = ag2_buf[i]
    for copy in a_sends + ss_sends + gather.sends + act_sends + gather2.sends:
        copy.wait_send()


def store_kernel(
    pos_ref, x2_ref, kn_ref, vn_ref, k_in, v_in, out_ref, k_out, v_out, k_buf, v_buf,
    pos, x2, pos_sem, x_sem, k_sem, v_sem,
):
    rows, keys = k_out.shape[:2]
    load = pltpu.make_async_copy(pos_ref, pos, pos_sem)
    load.start()
    x2[...] = x2_ref[...].astype(BF16)
    out = pltpu.make_async_copy(x2, out_ref, x_sem)
    out.start()
    load.wait()
    first_slot = lax.axis_index("sp") * (keys // 2)
    row16 = lax.broadcasted_iota(jnp.int32, (16, 128), 0)

    def put(ref, new, b, ploc):
        start = pl.multiple_of((jnp.clip(ploc * 2, 0, keys - 2) // 16) * 16, 16)
        block = ref[b, pl.ds(start, 16), :].astype(F32)
        at = row16 + start
        block = jnp.where(at == ploc * 2, new[0, b:b + 1, :], block)
        block = jnp.where(at == ploc * 2 + 1, new[1, b:b + 1, :], block)
        ref[b, pl.ds(start, 16), :] = block.astype(BF16)

    copies = [out]
    for b in range(rows):
        ploc = pos[b] - first_slot
        put(k_buf, kn_ref, b, ploc)
        copies.append(pltpu.make_async_copy(k_buf.at[b], k_out.at[b], k_sem.at[b]))
        copies[-1].start()
        put(v_buf, vn_ref, b, ploc)
        copies.append(pltpu.make_async_copy(v_buf.at[b], v_out.at[b], v_sem.at[b]))
        copies[-1].start()
    for copy in copies:
        copy.wait()


def solution(mesh):
    cache_spec = P("dp", "sp", "tp", None)
    vmem = pl.BlockSpec(memory_space=pltpu.VMEM)
    hbm = pl.BlockSpec(memory_space=pltpu.HBM)

    def in_hbm(*arrays):
        return tuple(pltpu.with_memory_space_constraint(a, pltpu.HBM) for a in arrays)

    def local_step(hidden, positions, norm_attn, norm_mlp, w_qkv, w_out, w_gate_up, w_down, k_cache, v_cache):
        rows, block_len, kv_local, head_dim = k_cache.shape
        dim = hidden.shape[1]
        flat = (rows, block_len * kv_local, head_dim)
        freq = ROPE_BASE ** (-np.arange(0, head_dim, 2, dtype=np.float64) / head_dim)
        freq = jnp.asarray(np.concatenate([freq, freq])[None].astype(np.float32))
        units = w_down.shape[0] // SP
        fresh = (kv_local, rows, head_dim)
        x2, k_mid, v_mid, k_new, v_new = pl.pallas_call(
            layer_kernel,
            out_shape=(
                pltpu.VMEM((rows, dim), F32),
                pltpu.VMEM(flat, BF16),
                pltpu.VMEM(flat, BF16),
                pltpu.VMEM(fresh, F32),
                pltpu.VMEM(fresh, F32),
            ),
            in_specs=[hbm] * 11,
            out_specs=(vmem,) * 5,
            scratch_shapes=[
                pltpu.SMEM((rows,), jnp.int32),
                pltpu.VMEM((1, head_dim), F32),
                pltpu.VMEM((rows, dim), BF16),
                pltpu.VMEM((1, dim), F32),
                pltpu.VMEM((1, dim), F32),
                pltpu.VMEM((W_CHUNKS, dim // W_CHUNKS, w_qkv.shape[1]), BF16),
                pltpu.VMEM((TP, 1024, 256), BF16),
                pltpu.VMEM((dim, 2 * units), BF16),
                pltpu.VMEM((SP, units, 1024), BF16),
                pltpu.VMEM((rows, dim), BF16),
                pltpu.VMEM((rows, 8, 128), F32),
                pltpu.VMEM((rows + 2, 8, 128), F32),
                pltpu.VMEM((3, rows + 2, 8, 128), F32),
                pltpu.VMEM((rows, 8, 128), F32),
                pltpu.VMEM((rows, 1024), BF16),
                pltpu.VMEM((TP, rows, 256), F32),
                pltpu.VMEM((TP, rows, 256), F32),
                pltpu.VMEM((16, rows, 256), F32),
                pltpu.VMEM((16, 1, 128), F32),
                pltpu.VMEM((SP, rows, 1024), BF16),
                pltpu.VMEM((SP, rows, units), F32),
                pltpu.VMEM((TP, rows, 256), F32),
                pltpu.VMEM((TP, rows, 256), F32),
                pltpu.VMEM((TP, rows, 256), F32),
                pltpu.VMEM((16, rows, 256), F32),
                pltpu.SemaphoreType.DMA((5,)),
                pltpu.SemaphoreType.DMA((W_CHUNKS,)),
                pltpu.SemaphoreType.DMA((rows,)),
                pltpu.SemaphoreType.DMA((rows,)),
                pltpu.SemaphoreType.DMA((TP,)),
                pltpu.SemaphoreType.DMA((8, 2)),
                pltpu.SemaphoreType.DMA((SP,)),
                pltpu.SemaphoreType.DMA((rows // GROUP, 2, 3)),
                pltpu.SemaphoreType.DMA((2, 4)),
                pltpu.SemaphoreType.DMA((2, 15)),
                pltpu.SemaphoreType.DMA((2, 15)),
                pltpu.SemaphoreType.DMA((2, 3)),
                pltpu.SemaphoreType.DMA((2, 4)),
                pltpu.SemaphoreType.DMA((2, 15)),
            ],
            compiler_params=pltpu.CompilerParams(
                collective_id=0, has_side_effects=True, vmem_limit_bytes=44 * 2 ** 20
            ),
            cost_estimate=pl.CostEstimate(flops=4 * 10 ** 9, bytes_accessed=6 * 10 ** 7, transcendentals=10 ** 6),
        )(*in_hbm(
            positions, freq, hidden, norm_attn.reshape(1, dim), norm_mlp.reshape(1, dim), w_qkv,
            k_cache.reshape(flat), v_cache.reshape(flat), w_out, w_gate_up, w_down,
        ))
        result, k_upd, v_upd, _, _ = pl.pallas_call(
            store_kernel,
            out_shape=(
                jax.ShapeDtypeStruct((rows, dim), BF16),
                jax.ShapeDtypeStruct(flat, BF16),
                jax.ShapeDtypeStruct(flat, BF16),
                pltpu.VMEM(flat, BF16),
                pltpu.VMEM(flat, BF16),
            ),
            in_specs=[hbm] + [vmem] * 5,
            out_specs=(hbm, hbm, hbm, vmem, vmem),
            input_output_aliases={4: 3, 5: 4},
            scratch_shapes=[
                pltpu.SMEM((rows,), jnp.int32),
                pltpu.VMEM((rows, dim), BF16),
                pltpu.SemaphoreType.DMA,
                pltpu.SemaphoreType.DMA,
                pltpu.SemaphoreType.DMA((rows,)),
                pltpu.SemaphoreType.DMA((rows,)),
            ],
            compiler_params=pltpu.CompilerParams(vmem_limit_bytes=8 * 2 ** 20),
            cost_estimate=pl.CostEstimate(flops=10 ** 8, bytes_accessed=2 * 10 ** 7, transcendentals=0),
        )(*in_hbm(positions), x2, k_new, v_new, k_mid, v_mid)
        return result, k_upd.reshape(k_cache.shape), v_upd.reshape(v_cache.shape)

    return jax.shard_map(
        local_step, mesh=mesh,
        in_specs=(P("dp", None), P("dp"), P(None), P(None), P(None, "tp"), P("tp", None), P(None, "tp"), P("tp", None), cache_spec, cache_spec),
        out_specs=(P("dp", None), cache_spec, cache_spec), check_vma=False,
    )
```

```python
import jax
import jax.numpy as jnp
import numpy as np
from jax import lax
from jax.experimental import pallas as pl
from jax.experimental.pallas import tpu as pltpu
from jax.sharding import PartitionSpec as P

WINDOW = 2047
ROPE_BASE = 10000.0
NORM_EPS = 1e-5
MESH = pl.DeviceIdType.MESH
F32 = jnp.float32
BF16 = jnp.bfloat16
NEG = float(jnp.finfo(jnp.float32).min)

TP = 4
SP = 4
W_CHUNKS = 8
GROUP = 4
OFFSETS = (
    (0, 1), (0, 3), (1, 1), (2, 1), (1, 3), (3, 1), (2, 3), (3, 3),
    (0, 2), (1, 0), (2, 0), (1, 2), (3, 0), (2, 2), (3, 2),
)
VIA = {off: off if off[1] & 1 else (0, 1) for off in OFFSETS}


def add_offsets(a, b):
    return (a[0] ^ b[0], a[1] ^ b[1])


def layer_kernel(
    pos_ref, freq_ref, x_ref, gain_ref, gain2_ref, wq_ref, k_ref, v_ref, wo_ref, wg_ref, wd_ref,
    out_ref, k_buf, v_buf, kn_buf, vn_buf, pos,
    freq, x_buf, gain, gain2, wq_buf, wo_buf, wg_buf, wd_buf,
    r_buf, q_buf, part, part_rx, o_buf, ob_buf, rs_tx, rs_rx, ag_buf, ss_buf, r2_buf,
    act_buf, dn_buf, rs2_tx, rs2_rx, ag2_buf,
    in_sem, wq_sem, k_sem, v_sem, wo_sem, wg_sem, wd_sem,
    a_sem, b_sem, s_sem, g_sem, c_sem, d_sem, e_sem, send_sem,
):
    dp, t, s = lax.axis_index("dp"), lax.axis_index("tp"), lax.axis_index("sp")
    rows, dim = x_ref.shape
    keys = k_ref.shape[1]
    units = wg_buf.shape[1] // 2
    ffn = wd_ref.shape[0]
    depth = dim // W_CHUNKS

    def peer(off):
        return (dp, t ^ off[0], s ^ off[1])

    def piece_of(off):
        return (s ^ off[1] ^ 1) * TP + (t ^ off[0])

    me = piece_of((0, 0))

    def remote(src, dst, phase, recv, off):
        return pltpu.make_async_remote_copy(
            src_ref=src, dst_ref=dst, send_sem=send_sem.at[phase], recv_sem=recv,
            device_id=peer(off), device_id_type=MESH,
        )

    def wait_bytes(ref, sem):
        pltpu.make_async_copy(ref, ref, sem).wait()

    small = [
        pltpu.make_async_copy(src, dst, in_sem.at[i])
        for i, (src, dst) in enumerate((
            (x_ref, x_buf), (gain_ref, gain), (freq_ref, freq), (pos_ref, pos), (gain2_ref, gain2)
        ))
    ]
    for copy in small:
        copy.start()

    def wq_copy(c):
        return pltpu.make_async_copy(wq_ref.at[pl.ds(c * depth, depth)], wq_buf.at[c], wq_sem.at[c])

    def k_copy(g):
        at = pl.ds(g * GROUP, GROUP)
        return pltpu.make_async_copy(k_ref.at[at], k_buf.at[at], k_sem.at[g])

    def v_copy(g):
        at = pl.ds(g * GROUP, GROUP)
        return pltpu.make_async_copy(v_ref.at[at], v_buf.at[at], v_sem.at[g])

    def start_wo():
        for d in range(TP):
            col = pl.multiple_of((s * TP + d) * 256, 256)
            pltpu.make_async_copy(wo_ref.at[:, pl.ds(col, 256)], wo_buf.at[d], wo_sem).start()

    def start_wg(c):
        for half in range(2):
            col = pl.multiple_of(half * ffn + s * units, 128)
            pltpu.make_async_copy(
                wg_ref.at[pl.ds(c * 1024, 1024), pl.ds(col, units)],
                wg_buf.at[pl.ds(c * 1024, 1024), pl.ds(half * units, units)],
                wg_sem,
            ).start()

    def start_wd():
        for c in range(SP):
            col = pl.multiple_of(s * 1024, 1024)
            pltpu.make_async_copy(
                wd_ref.at[pl.ds(c * units, units), pl.ds(col, 1024)], wd_buf.at[c], wd_sem
            ).start()

    wq_copy(0).start()
    wq_copy(1).start()
    barrier = pltpu.get_barrier_semaphore()
    for off in OFFSETS:
        pl.semaphore_signal(barrier, inc=1, device_id=peer(off), device_id_type=MESH)

    for copy in small:
        copy.wait()
    for c in range(2, W_CHUNKS):
        wq_copy(c).start()
    x = x_buf[...].astype(F32)
    scale = lax.rsqrt(jnp.mean(x * x, axis=-1, keepdims=True) + NORM_EPS)
    r_buf[...] = (x * scale * gain[...]).astype(BF16)
    row_id = lax.broadcasted_iota(jnp.int32, (rows, 128), 0)
    lane_id = lax.broadcasted_iota(jnp.int32, (rows, 128), 1)
    diag = row_id == lane_id

    qkv = None
    for c in range(W_CHUNKS):
        wq_copy(c).wait()
        if c >= W_CHUNKS - GROUP:
            k_copy(c - W_CHUNKS + GROUP).start()
            v_copy(c - W_CHUNKS + GROUP).start()
        term = jnp.dot(r_buf[:, c * depth:(c + 1) * depth], wq_buf[c], preferred_element_type=F32)
        qkv = term if qkv is None else qkv + term
        if c == 1:
            pos_col = jnp.zeros((rows, 128), jnp.int32)
            for b in range(rows):
                pos_col = jnp.where(row_id == b, pos[b], pos_col)
            angle = pos_col.astype(F32) * freq[...]
            cos = jnp.cos(angle)
            sin = jnp.sin(angle)
            sin = jnp.where(lane_id < 64, -sin, sin)

    def rotate(vals):
        out = vals * cos + pltpu.roll(vals, 64, 1) * sin
        return out.astype(BF16).astype(F32)

    for kv in range(2):
        base = kv * 768
        for h in range(4):
            q_buf[:, kv * 4 + h, :] = rotate(qkv[:, base + h * 128:base + (h + 1) * 128])
        kn_buf[kv] = rotate(qkv[:, base + 512:base + 640])
        vn_buf[kv] = qkv[:, base + 640:base + 768].astype(BF16).astype(F32)

    pl.semaphore_wait(barrier, len(OFFSETS))
    first_slot = s * (keys // 2)
    lane = lax.broadcasted_iota(jnp.int32, (8, keys), 1)
    head = lax.broadcasted_iota(jnp.int32, (8, keys), 0)
    own = (lane & 1) == (head >> 2)
    slot_id = lane >> 1
    lane8 = lax.broadcasted_iota(jnp.int32, (8, 128), 1)
    sub8 = lax.broadcasted_iota(jnp.int32, (8, 128), 0)
    low_heads = sub8 < 4
    scale = 128 ** -0.5

    def new_rows(buf, b):
        return jnp.where(low_heads, buf[0, pl.ds(b, 1), :], buf[1, pl.ds(b, 1), :])

    def a_rows(g):
        return pl.ds(g * GROUP, GROUP + (2 if g == rows // GROUP - 1 else 0))

    groups = rows // GROUP

    def a_copy(g, k, off):
        recv = a_sem.at[g if k == 2 else groups]
        return remote(part.at[a_rows(g)], part_rx.at[k, a_rows(g)], 0, recv, off)

    def a_forward(g):
        return remote(part_rx.at[2, a_rows(g)], part_rx.at[1, a_rows(g)], 0, a_sem.at[groups + 1], (0, 1))

    m_all = jnp.zeros((8, 128), F32)
    l_all = jnp.zeros((8, 128), F32)
    n_all = jnp.zeros((8, 128), F32)
    for g in range(rows // GROUP):
        ids = range(g * GROUP, (g + 1) * GROUP)
        k_copy(g).wait()
        v_copy(g).wait()
        scores = []
        for b in ids:
            q = q_buf[b]
            scores.append(lax.dot_general(
                q.astype(BF16), k_buf[b], (((1,), (1,)), ((), ())), preferred_element_type=F32
            ))
            fresh = jnp.sum(q * new_rows(kn_buf, b), axis=-1, keepdims=True) * scale
            n_all = jnp.where(lane8 == sub8 + b * 8, fresh, n_all)
        probs = []
        for b, sc in zip(ids, scores):
            ploc = pos[b] - first_slot
            mask = own & (slot_id < ploc) & (slot_id >= ploc - WINDOW)
            sc = jnp.where(mask, sc * scale, NEG)
            m = jnp.max(sc, axis=-1, keepdims=True)
            w = jnp.where(mask, jnp.exp(sc - m), 0.0)
            l = jnp.sum(w, axis=-1, keepdims=True)
            at = lane8 == sub8 + b * 8
            m_all = jnp.where(at, m, m_all)
            l_all = jnp.where(at, l, l_all)
            probs.append(w.astype(BF16))
        for b, w in zip(ids, probs):
            part[b] = jnp.dot(w, v_buf[b], preferred_element_type=F32)
        if g == rows // GROUP - 1:
            part[rows] = m_all
            part[rows + 1] = l_all
        for k, off in ((2, (0, 3)), (0, (0, 1))):
            a_copy(g, k, off).start()
        if g == 1:
            start_wo()
        if g == 2:
            start_wg(0)
            start_wg(1)
        if g == 3:
            start_wg(2)
            start_wg(3)
            start_wd()

    for g in range(rows // GROUP):
        a_copy(g, 2, (0, 3)).wait_recv()
        a_forward(g).start()
    wait_bytes(part_rx.at[0], a_sem.at[groups])
    wait_bytes(part_rx.at[1], a_sem.at[groups + 1])
    parts = [part, part_rx.at[0], part_rx.at[1], part_rx.at[2]]
    top = n_all
    for p in parts:
        top = jnp.maximum(top, p[rows])
    facs = [jnp.exp(p[rows] - top) for p in parts]
    fresh = jnp.exp(n_all - top)
    total = fresh
    for p, f in zip(parts, facs):
        total = total + p[rows + 1] * f
    inv = 1.0 / total
    facs = [f * inv for f in facs]
    fresh = fresh * inv
    for b in range(rows):
        at = lane8 == sub8 + b * 8
        o = new_rows(vn_buf, b) * jnp.sum(jnp.where(at, fresh, 0.0), axis=-1, keepdims=True)
        for p, f in zip(parts, facs):
            o = o + p[b] * jnp.sum(jnp.where(at, f, 0.0), axis=-1, keepdims=True)
        o_buf[b] = o
    for h in range(8):
        ob_buf[:, h * 128:(h + 1) * 128] = o_buf[:, h, :].astype(BF16)

    def reduce_scatter(make_term, tx, rx, phase, sem):
        for dt in (3, 2, 1, 0):
            tx[dt] = make_term(t ^ dt)
            remote(tx.at[dt], rx.at[dt], phase, sem, (dt, 1)).start()
        wait_bytes(rx, sem)
        return rx[0] + rx[1] + rx[2] + rx[3]

    wait_bytes(wo_buf, wo_sem)
    o_all = ob_buf[...]

    def out_term(d):
        return jnp.dot(o_all, wo_buf[d], preferred_element_type=F32).astype(BF16).astype(F32)

    my_cols = pl.ds(pl.multiple_of(me * 256, 256), 256)
    mid = x_buf[:, my_cols].astype(F32) + reduce_scatter(out_term, rs_tx, rs_rx, 1, b_sem)
    ag_buf[me] = mid
    sq = jnp.sum(mid * mid, axis=-1, keepdims=True)
    ss_buf[me] = jnp.sum(jnp.where(diag, sq, 0.0), axis=0, keepdims=True)

    class Gather:
        def __init__(self, buf, sems, phase):
            self.buf, self.sems, self.phase = buf, sems, phase

        def send(self, have):
            for k in reversed(range(len(OFFSETS))):
                off = OFFSETS[k]
                if add_offsets(off, VIA[off]) == have:
                    slot = piece_of(have)
                    recv = self.sems.at[k if k < 8 else 8 + off[1] // 2]
                    remote(self.buf.at[slot], self.buf.at[slot], self.phase, recv, VIA[off]).start()

        def wait(self, off):
            slot = piece_of(off)
            k = OFFSETS.index(off)
            remote(self.buf.at[slot], self.buf.at[slot], self.phase, self.sems.at[k], off).wait_recv()
            self.send(off)

        def wait_block(self, ds):
            wait_bytes(self.buf.at[pl.ds(0, 3 if ds == 0 else 4)], self.sems.at[8 + ds // 2])

    for off in sorted(OFFSETS, key=lambda o: -o[0]):
        remote(ss_buf.at[me], ss_buf.at[me], 2, s_sem, off).start()
    gather = Gather(ag_buf, g_sem, 3)
    gather.send((0, 0))
    for off in OFFSETS[:8]:
        gather.wait(off)
    wait_bytes(ss_buf.at[pl.ds(0, len(OFFSETS))], s_sem)
    tot = jnp.sum(ss_buf[...], axis=0)
    mean_sq = jnp.sum(jnp.where(diag, tot, 0.0), axis=-1, keepdims=True) / dim
    rstd = lax.rsqrt(mean_sq + NORM_EPS)
    wait_bytes(wg_buf, wg_sem)

    def gate_up(ds):
        block = s ^ ds ^ 1
        for j in range(TP):
            at = pl.ds(pl.multiple_of((block * TP + j) * 256, 256), 256)
            r2_buf[ds, :, j * 256:(j + 1) * 256] = (ag_buf[block * TP + j] * rstd * gain2[:, at]).astype(BF16)
        at = pl.ds(pl.multiple_of(block * 1024, 1024), 1024)
        return jnp.dot(r2_buf[ds], wg_buf[at, :], preferred_element_type=F32)

    hid = gate_up(1) + gate_up(3)
    gather.wait_block(0)
    hid = hid + gate_up(0)
    gather.wait_block(2)
    hid = hid + gate_up(2)
    gate, up = hid[:, :units], hid[:, units:]
    act_buf[s] = (gate * jax.nn.sigmoid(gate) * up).astype(BF16).astype(F32)

    def act_send(slot, k, off):
        remote(act_buf.at[slot], act_buf.at[slot], 4, c_sem.at[k], off).start()

    act_send(s, 2, (0, 3))
    act_send(s, 0, (0, 1))
    wait_bytes(wd_buf, wd_sem)
    down = jnp.dot(act_buf[s].astype(BF16), wd_buf[s], preferred_element_type=F32)
    for k in (0, 2, 1):
        slot = s ^ (k + 1)
        remote(act_buf.at[slot], act_buf.at[slot], 4, c_sem.at[k], (0, 1)).wait_recv()
        if k == 2:
            act_send(slot, 1, (0, 1))
        down = down + jnp.dot(act_buf[slot].astype(BF16), wd_buf[slot], preferred_element_type=F32)
    down = down.astype(BF16).astype(F32)
    for d in range(TP):
        dn_buf[d] = down[:, d * 256:(d + 1) * 256]

    def down_term(d):
        return dn_buf[d]

    ag2_buf[me] = mid + reduce_scatter(down_term, rs2_tx, rs2_rx, 5, d_sem)
    gather2 = Gather(ag2_buf, e_sem, 6)
    gather2.send((0, 0))
    for off in OFFSETS[:8]:
        gather2.wait(off)
    gather2.wait_block(0)
    gather2.wait_block(2)
    for i in range(16):
        out_ref[:, i * 256:(i + 1) * 256] = ag2_buf[i]
    sent = (
        part_rx, rs_tx, ss_buf.at[pl.ds(0, 15)], ag_buf.at[pl.ds(0, 15)], act_buf.at[pl.ds(0, 3)],
        rs2_tx, ag2_buf.at[pl.ds(0, 15)],
    )
    for phase, ref in enumerate(sent):
        wait_bytes(ref, send_sem.at[phase])


def store_kernel(
    pos, x2_ref, kn_ref, vn_ref, k_in, v_in, out_ref, k_out, v_out, k_buf, v_buf, x2, x_sem, k_sem, v_sem
):
    rows, keys = k_out.shape[:2]
    x2[...] = x2_ref[...].astype(BF16)
    out = pltpu.make_async_copy(x2, out_ref, x_sem)
    out.start()
    first_slot = lax.axis_index("sp") * (keys // 2)
    row16 = lax.broadcasted_iota(jnp.int32, (16, 128), 0)

    def put(ref, new, b, ploc):
        start = pl.multiple_of((jnp.clip(ploc * 2, 0, keys - 2) // 16) * 16, 16)
        block = ref[b, pl.ds(start, 16), :].astype(F32)
        at = row16 + start
        block = jnp.where(at == ploc * 2, new[0, b:b + 1, :], block)
        block = jnp.where(at == ploc * 2 + 1, new[1, b:b + 1, :], block)
        ref[b, pl.ds(start, 16), :] = block.astype(BF16)

    for b in range(rows):
        ploc = pos[b] - first_slot
        put(k_buf, kn_ref, b, ploc)
        pltpu.make_async_copy(k_buf.at[b], k_out.at[b], k_sem).start()
        put(v_buf, vn_ref, b, ploc)
        pltpu.make_async_copy(v_buf.at[b], v_out.at[b], v_sem).start()
    out.wait()
    pltpu.make_async_copy(k_buf, k_out, k_sem).wait()
    pltpu.make_async_copy(v_buf, v_out, v_sem).wait()


def solution(mesh):
    cache_spec = P("dp", "sp", "tp", None)
    vmem = pl.BlockSpec(memory_space=pltpu.VMEM)
    smem = pl.BlockSpec(memory_space=pltpu.SMEM)
    hbm = pl.BlockSpec(memory_space=pltpu.HBM)

    def in_hbm(*arrays):
        return tuple(pltpu.with_memory_space_constraint(a, pltpu.HBM) for a in arrays)

    def local_step(hidden, positions, norm_attn, norm_mlp, w_qkv, w_out, w_gate_up, w_down, k_cache, v_cache):
        rows, block_len, kv_local, head_dim = k_cache.shape
        dim = hidden.shape[1]
        flat = (rows, block_len * kv_local, head_dim)
        freq = ROPE_BASE ** (-np.arange(0, head_dim, 2, dtype=np.float64) / head_dim)
        freq = jnp.asarray(np.concatenate([freq, freq])[None].astype(np.float32))
        units = w_down.shape[0] // SP
        fresh = (kv_local, rows, head_dim)
        x2, k_mid, v_mid, k_new, v_new, pos = pl.pallas_call(
            layer_kernel,
            out_shape=(
                pltpu.VMEM((rows, dim), F32),
                pltpu.VMEM(flat, BF16),
                pltpu.VMEM(flat, BF16),
                pltpu.VMEM(fresh, F32),
                pltpu.VMEM(fresh, F32),
                pltpu.SMEM((rows,), jnp.int32),
            ),
            in_specs=[hbm] * 11,
            out_specs=(vmem,) * 5 + (smem,),
            scratch_shapes=[
                pltpu.VMEM((1, head_dim), F32),
                pltpu.VMEM((rows, dim), BF16),
                pltpu.VMEM((1, dim), F32),
                pltpu.VMEM((1, dim), F32),
                pltpu.VMEM((W_CHUNKS, dim // W_CHUNKS, w_qkv.shape[1]), BF16),
                pltpu.VMEM((TP, 1024, 256), BF16),
                pltpu.VMEM((dim, 2 * units), BF16),
                pltpu.VMEM((SP, units, 1024), BF16),
                pltpu.VMEM((rows, dim), BF16),
                pltpu.VMEM((rows, 8, 128), F32),
                pltpu.VMEM((rows + 2, 8, 128), F32),
                pltpu.VMEM((3, rows + 2, 8, 128), F32),
                pltpu.VMEM((rows, 8, 128), F32),
                pltpu.VMEM((rows, 1024), BF16),
                pltpu.VMEM((TP, rows, 256), F32),
                pltpu.VMEM((TP, rows, 256), F32),
                pltpu.VMEM((16, rows, 256), F32),
                pltpu.VMEM((16, 1, 128), F32),
                pltpu.VMEM((SP, rows, 1024), BF16),
                pltpu.VMEM((SP, rows, units), F32),
                pltpu.VMEM((TP, rows, 256), F32),
                pltpu.VMEM((TP, rows, 256), F32),
                pltpu.VMEM((TP, rows, 256), F32),
                pltpu.VMEM((16, rows, 256), F32),
                pltpu.SemaphoreType.DMA((5,)),
                pltpu.SemaphoreType.DMA((W_CHUNKS,)),
                pltpu.SemaphoreType.DMA((rows // GROUP,)),
                pltpu.SemaphoreType.DMA((rows // GROUP,)),
                pltpu.SemaphoreType.DMA,
                pltpu.SemaphoreType.DMA,
                pltpu.SemaphoreType.DMA,
                pltpu.SemaphoreType.DMA((rows // GROUP + 2,)),
                pltpu.SemaphoreType.DMA,
                pltpu.SemaphoreType.DMA,
                pltpu.SemaphoreType.DMA((10,)),
                pltpu.SemaphoreType.DMA((3,)),
                pltpu.SemaphoreType.DMA,
                pltpu.SemaphoreType.DMA((10,)),
                pltpu.SemaphoreType.DMA((7,)),
            ],
            compiler_params=pltpu.CompilerParams(
                collective_id=0, has_side_effects=True, vmem_limit_bytes=44 * 2 ** 20
            ),
            cost_estimate=pl.CostEstimate(flops=4 * 10 ** 9, bytes_accessed=6 * 10 ** 7, transcendentals=10 ** 6),
        )(*in_hbm(
            positions, freq, hidden, norm_attn.reshape(1, dim), norm_mlp.reshape(1, dim), w_qkv,
            k_cache.reshape(flat), v_cache.reshape(flat), w_out, w_gate_up, w_down,
        ))
        result, k_upd, v_upd, _, _ = pl.pallas_call(
            store_kernel,
            out_shape=(
                jax.ShapeDtypeStruct((rows, dim), BF16),
                jax.ShapeDtypeStruct(flat, BF16),
                jax.ShapeDtypeStruct(flat, BF16),
                pltpu.VMEM(flat, BF16),
                pltpu.VMEM(flat, BF16),
            ),
            in_specs=[smem] + [vmem] * 5,
            out_specs=(hbm, hbm, hbm, vmem, vmem),
            input_output_aliases={4: 3, 5: 4},
            scratch_shapes=[
                pltpu.VMEM((rows, dim), BF16),
                pltpu.SemaphoreType.DMA,
                pltpu.SemaphoreType.DMA,
                pltpu.SemaphoreType.DMA,
            ],
            compiler_params=pltpu.CompilerParams(vmem_limit_bytes=8 * 2 ** 20),
            cost_estimate=pl.CostEstimate(flops=10 ** 8, bytes_accessed=2 * 10 ** 7, transcendentals=0),
        )(pos, x2, k_new, v_new, k_mid, v_mid)
        return result, k_upd.reshape(k_cache.shape), v_upd.reshape(v_cache.shape)

    return jax.shard_map(
        local_step, mesh=mesh,
        in_specs=(P("dp", None), P("dp"), P(None), P(None), P(None, "tp"), P("tp", None), P(None, "tp"), P("tp", None), cache_spec, cache_spec),
        out_specs=(P("dp", None), cache_spec, cache_spec), check_vma=False,
    )
```

```python
import jax
import jax.numpy as jnp
import numpy as np
from jax import lax
from jax.experimental import pallas as pl
from jax.experimental.pallas import tpu as pltpu
from jax.sharding import PartitionSpec as P

WINDOW = 2047
ROPE_BASE = 10000.0
NORM_EPS = 1e-5
MESH = pl.DeviceIdType.MESH
F32 = jnp.float32
BF16 = jnp.bfloat16
NEG = float(jnp.finfo(jnp.float32).min)

TP = 4
SP = 4
W_CHUNKS = 4
GROUP = 2
FLIGHT = 3
OFFSETS = (
    (0, 1), (0, 3), (1, 1), (2, 1), (1, 3), (3, 1), (2, 3), (3, 3),
    (0, 2), (1, 0), (2, 0), (1, 2), (3, 0), (2, 2), (3, 2),
)
VIA = {off: off if off[1] & 1 else (0, 1) for off in OFFSETS}


def add_offsets(a, b):
    return (a[0] ^ b[0], a[1] ^ b[1])


def layer_kernel(
    pos_ref, freq_ref, x_ref, gain_ref, gain2_ref, wq_ref, k_ref, v_ref, wo_ref, wg_ref, wd_ref,
    out_ref, k_buf, v_buf, kn_buf, vn_buf, pos,
    freq, x_buf, gain, gain2, wo_buf, wg_buf, wd_buf,
    r_buf, qkv_buf, q_buf, part, part_rx, o_buf, ob_buf, rs_tx, rs_rx, ag_buf, ss_buf,
    act_buf, dn_buf, rs2_tx, rs2_rx, ag2_buf,
    in_sem, wq_sem, k_sem, v_sem, wo_sem, wg_sem, wd_sem,
    a_sem, b_sem, s_sem, g_sem, c_sem, d_sem, e_sem, q_sem, send_sem,
):
    dp, t, s = lax.axis_index("dp"), lax.axis_index("tp"), lax.axis_index("sp")
    rows, dim = x_ref.shape
    keys = k_ref.shape[1]
    units = wg_buf.shape[1] // 2
    ffn = wd_ref.shape[0]
    depth = dim // W_CHUNKS
    core = s & 1
    q_cols = wq_ref.shape[1] // 2
    wq_buf = wg_buf.at[:, pl.ds(0, q_cols)]

    def peer(off):
        return (dp, t ^ off[0], s ^ off[1])

    def piece_of(off):
        return (s ^ off[1] ^ 1) * TP + (t ^ off[0])

    me = piece_of((0, 0))

    def remote(src, dst, phase, recv, off):
        return pltpu.make_async_remote_copy(
            src_ref=src, dst_ref=dst, send_sem=send_sem.at[phase], recv_sem=recv,
            device_id=peer(off), device_id_type=MESH,
        )

    def wait_bytes(ref, sem):
        pltpu.make_async_copy(ref, ref, sem).wait()

    small = [
        pltpu.make_async_copy(src, dst, in_sem.at[i])
        for i, (src, dst) in enumerate((
            (x_ref, x_buf), (gain_ref, gain), (freq_ref, freq), (pos_ref, pos), (gain2_ref, gain2)
        ))
    ]
    for copy in small:
        copy.start()

    def wq_copy(c):
        at = pl.ds(c * depth, depth)
        cols = pl.ds(pl.multiple_of(core * q_cols, 128), q_cols)
        return pltpu.make_async_copy(wq_ref.at[at, cols], wq_buf.at[at], wq_sem.at[c])

    def k_copy(g):
        at = pl.ds(g * GROUP, GROUP)
        return pltpu.make_async_copy(k_ref.at[at], k_buf.at[at], k_sem.at[g])

    def v_copy(g):
        at = pl.ds(g * GROUP, GROUP)
        return pltpu.make_async_copy(v_ref.at[at], v_buf.at[at], v_sem.at[g])

    def start_wo():
        for d in range(TP):
            col = pl.multiple_of((s * TP + d) * 256, 256)
            pltpu.make_async_copy(wo_ref.at[:, pl.ds(col, 256)], wo_buf.at[d], wo_sem).start()

    def start_wg(c):
        for half in range(2):
            col = pl.multiple_of(half * ffn + core * units, 128)
            pltpu.make_async_copy(
                wg_ref.at[pl.ds(c * 1024, 1024), pl.ds(col, units)],
                wg_buf.at[pl.ds(c * 1024, 1024), pl.ds(half * units, units)],
                wg_sem,
            ).start()

    def start_wd():
        for c in range(2):
            col = pl.multiple_of(s * 1024, 1024)
            pltpu.make_async_copy(
                wd_ref.at[pl.ds(c * units, units), pl.ds(col, 1024)], wd_buf.at[c], wd_sem
            ).start()

    def kv_loads(g):
        return [k_copy(g), v_copy(g)]

    loads = [[wq_copy(c)] for c in range(W_CHUNKS)] + [kv_loads(g) for g in range(rows // GROUP)]

    def start_load(i):
        if i < len(loads):
            for copy in loads[i]:
                copy.start()

    for i in range(FLIGHT):
        start_load(i)
    barrier = pltpu.get_barrier_semaphore()
    for off in OFFSETS:
        pl.semaphore_signal(barrier, inc=1, device_id=peer(off), device_id_type=MESH)

    for c in range(FLIGHT):
        wq_copy(c).wait()
        start_load(FLIGHT + c)
    for copy in small:
        copy.wait()
    x = x_buf[...].astype(F32)
    scale = lax.rsqrt(jnp.mean(x * x, axis=-1, keepdims=True) + NORM_EPS)
    r_buf[...] = (x * scale * gain[...]).astype(BF16)
    row_id = lax.broadcasted_iota(jnp.int32, (rows, 128), 0)
    lane_id = lax.broadcasted_iota(jnp.int32, (rows, 128), 1)
    diag = row_id == lane_id

    def qkv_term(c):
        at = pl.ds(c * depth, depth)
        return jnp.dot(r_buf[:, c * depth:(c + 1) * depth], wq_buf[at, :], preferred_element_type=F32)

    qkv = qkv_term(0)
    for c in range(1, FLIGHT):
        qkv = qkv + qkv_term(c)
    pos_col = jnp.zeros((rows, 128), jnp.int32)
    for b in range(rows):
        pos_col = jnp.where(row_id == b, pos[b], pos_col)
    angle = pos_col.astype(F32) * freq[...]
    cos = jnp.cos(angle)
    sin = jnp.sin(angle)
    sin = jnp.where(lane_id < 64, -sin, sin)
    for c in range(FLIGHT, W_CHUNKS):
        wq_copy(c).wait()
        start_load(FLIGHT + c)
        if c == W_CHUNKS - 1:
            start_load(FLIGHT + c + 1)
            start_load(FLIGHT + c + 2)
        qkv = qkv + qkv_term(c)

    qkv_buf[core] = qkv
    pl.semaphore_wait(barrier, len(OFFSETS))
    remote(qkv_buf.at[core], qkv_buf.at[core], 7, q_sem, (0, 1)).start()
    wait_bytes(qkv_buf.at[1 - core], q_sem)
    def rotate(vals):
        out = vals * cos + pltpu.roll(vals, 64, 1) * sin
        return out.astype(BF16).astype(F32)

    for kv in range(2):
        for h in range(4):
            q_buf[:, kv * 4 + h, :] = rotate(qkv_buf[kv, :, h * 128:(h + 1) * 128])
        kn_buf[kv] = rotate(qkv_buf[kv, :, 512:640])
        vn_buf[kv] = qkv_buf[kv, :, 640:768].astype(BF16).astype(F32)

    first_slot = s * (keys // 2)
    lane = lax.broadcasted_iota(jnp.int32, (8, keys), 1)
    head = lax.broadcasted_iota(jnp.int32, (8, keys), 0)
    own = (lane & 1) == (head >> 2)
    slot_id = lane >> 1
    lane8 = lax.broadcasted_iota(jnp.int32, (8, 128), 1)
    sub8 = lax.broadcasted_iota(jnp.int32, (8, 128), 0)
    low_heads = sub8 < 4
    scale = 128 ** -0.5

    def new_rows(buf, b):
        return jnp.where(low_heads, buf[0, pl.ds(b, 1), :], buf[1, pl.ds(b, 1), :])

    def a_rows(g):
        return pl.ds(g * GROUP, GROUP + (2 if g == rows // GROUP - 1 else 0))

    groups = rows // GROUP

    def a_copy(g, k, off):
        recv = a_sem.at[g if k == 2 else groups]
        return remote(part.at[a_rows(g)], part_rx.at[k, a_rows(g)], 0, recv, off)

    def a_forward(g):
        return remote(part_rx.at[2, a_rows(g)], part_rx.at[1, a_rows(g)], 0, a_sem.at[groups + 1], (0, 1))

    m_all = jnp.zeros((8, 128), F32)
    l_all = jnp.zeros((8, 128), F32)
    n_all = jnp.zeros((8, 128), F32)

    def group_scores(g):
        k_copy(g).wait()
        v_copy(g).wait()
        start_load(W_CHUNKS + FLIGHT + 2 + g)
        return [
            lax.dot_general(
                q_buf[b].astype(BF16), k_buf[b], (((1,), (1,)), ((), ())), preferred_element_type=F32
            )
            for b in range(g * GROUP, (g + 1) * GROUP)
        ]

    pending = group_scores(0)
    for g in range(groups):
        ids = range(g * GROUP, (g + 1) * GROUP)
        scores = pending
        if g + 1 < groups:
            pending = group_scores(g + 1)
        probs = []
        for b, sc in zip(ids, scores):
            fresh = jnp.sum(q_buf[b] * new_rows(kn_buf, b), axis=-1, keepdims=True) * scale
            ploc = pos[b] - first_slot
            mask = own & (slot_id < ploc) & (slot_id >= ploc - WINDOW)
            sc = jnp.where(mask, sc * scale, NEG)
            m = jnp.max(sc, axis=-1, keepdims=True)
            w = jnp.where(mask, jnp.exp(sc - m), 0.0)
            l = jnp.sum(w, axis=-1, keepdims=True)
            at = lane8 == sub8 + b * 8
            n_all = jnp.where(at, fresh, n_all)
            m_all = jnp.where(at, m, m_all)
            l_all = jnp.where(at, l, l_all)
            probs.append(w.astype(BF16))
        for b, w in zip(ids, probs):
            part[b] = jnp.dot(w, v_buf[b], preferred_element_type=F32)
        if g == rows // GROUP - 1:
            part[rows] = m_all
            part[rows + 1] = l_all
        for k, off in ((2, (0, 3)), (0, (0, 1))):
            a_copy(g, k, off).start()
        if g == groups - 2:
            start_wo()
    for c in range(4):
        start_wg(c)
    start_wd()

    for g in range(groups):
        a_copy(g, 2, (0, 3)).wait_recv()
        a_forward(g).start()
    wait_bytes(part_rx.at[0], a_sem.at[groups])
    wait_bytes(part_rx.at[1], a_sem.at[groups + 1])
    parts = [part, part_rx.at[0], part_rx.at[1], part_rx.at[2]]
    top = n_all
    for p in parts:
        top = jnp.maximum(top, p[rows])
    facs = [jnp.exp(p[rows] - top) for p in parts]
    fresh = jnp.exp(n_all - top)
    total = fresh
    for p, f in zip(parts, facs):
        total = total + p[rows + 1] * f
    inv = 1.0 / total
    facs = [f * inv for f in facs]
    fresh = fresh * inv
    for b in range(rows):
        at = lane8 == sub8 + b * 8
        o = new_rows(vn_buf, b) * jnp.sum(jnp.where(at, fresh, 0.0), axis=-1, keepdims=True)
        for p, f in zip(parts, facs):
            o = o + p[b] * jnp.sum(jnp.where(at, f, 0.0), axis=-1, keepdims=True)
        o_buf[b] = o
    for h in range(8):
        ob_buf[:, h * 128:(h + 1) * 128] = o_buf[:, h, :].astype(BF16)

    def reduce_scatter(make_term, tx, rx, phase, sem):
        for dts in ((3,), (2, 1, 0)):
            for dt in dts:
                tx[dt] = make_term(t ^ dt)
            for dt in dts:
                remote(tx.at[dt], rx.at[dt], phase, sem, (dt, 1)).start()
        wait_bytes(rx, sem)
        return rx[0] + rx[1] + rx[2] + rx[3]

    wait_bytes(wo_buf, wo_sem)
    o_all = ob_buf[...]

    def out_term(d):
        return jnp.dot(o_all, wo_buf[d], preferred_element_type=F32).astype(BF16).astype(F32)

    my_cols = pl.ds(pl.multiple_of(me * 256, 256), 256)
    mid = x_buf[:, my_cols].astype(F32) + reduce_scatter(out_term, rs_tx, rs_rx, 1, b_sem)
    ag_buf[me] = mid
    sq = jnp.sum(mid * mid, axis=-1, keepdims=True)
    ss_buf[me] = jnp.sum(jnp.where(diag, sq, 0.0), axis=0, keepdims=True)

    class Gather:
        def __init__(self, buf, sems, phase):
            self.buf, self.sems, self.phase = buf, sems, phase

        def send(self, have):
            for k in reversed(range(len(OFFSETS))):
                off = OFFSETS[k]
                if add_offsets(off, VIA[off]) == have:
                    slot = piece_of(have)
                    recv = self.sems.at[k if k < 8 else 8 + off[1] // 2]
                    remote(self.buf.at[slot], self.buf.at[slot], self.phase, recv, VIA[off]).start()

        def wait(self, off):
            slot = piece_of(off)
            k = OFFSETS.index(off)
            remote(self.buf.at[slot], self.buf.at[slot], self.phase, self.sems.at[k], off).wait_recv()
            self.send(off)

        def wait_block(self, ds):
            wait_bytes(self.buf.at[pl.ds(0, 3 if ds == 0 else 4)], self.sems.at[8 + ds // 2])

    for off in sorted(OFFSETS, key=lambda o: -o[0]):
        remote(ss_buf.at[me], ss_buf.at[me], 2, s_sem, off).start()
    gather = Gather(ag_buf, g_sem, 3)
    gather.send((0, 0))
    for off in OFFSETS[:3]:
        gather.wait(off)
    wait_bytes(ss_buf.at[pl.ds(0, len(OFFSETS))], s_sem)
    tot = jnp.sum(ss_buf[...], axis=0)
    mean_sq = jnp.sum(jnp.where(diag, tot, 0.0), axis=-1, keepdims=True) / dim
    rstd = lax.rsqrt(mean_sq + NORM_EPS)
    wait_bytes(wg_buf, wg_sem)

    def gate_up(offs):
        out = None
        for off in offs:
            slot = piece_of(off)
            at = pl.ds(pl.multiple_of(slot * 256, 256), 256)
            r2 = (ag_buf[slot] * rstd * gain2[:, at]).astype(BF16)
            term = jnp.dot(r2, wg_buf[at, :], preferred_element_type=F32)
            out = term if out is None else out + term
        return out

    hid = gate_up(((0, 0),) + OFFSETS[:3])
    for off in OFFSETS[3:8]:
        gather.wait(off)
    hid = hid + gate_up(OFFSETS[3:8])
    gather.wait_block(0)
    gather.wait_block(2)
    hid = hid + gate_up(OFFSETS[8:])
    gate, up = hid[:, :units], hid[:, units:]
    act_buf[core] = (gate * jax.nn.sigmoid(gate) * up).astype(BF16).astype(F32)

    remote(act_buf.at[core], act_buf.at[core], 4, c_sem, (0, 1)).start()
    wait_bytes(wd_buf, wd_sem)
    down = jnp.dot(act_buf[core].astype(BF16), wd_buf[core], preferred_element_type=F32)
    wait_bytes(act_buf.at[1 - core], c_sem)
    down = down + jnp.dot(act_buf[1 - core].astype(BF16), wd_buf[1 - core], preferred_element_type=F32)
    down = down.astype(BF16).astype(F32)
    for d in range(TP):
        dn_buf[d] = down[:, d * 256:(d + 1) * 256]

    def down_term(d):
        return dn_buf[d]

    ag2_buf[me] = mid + reduce_scatter(down_term, rs2_tx, rs2_rx, 5, d_sem)
    gather2 = Gather(ag2_buf, e_sem, 6)
    gather2.send((0, 0))
    for off in OFFSETS[:8]:
        gather2.wait(off)
    gather2.wait_block(0)
    gather2.wait_block(2)
    for i in range(16):
        out_ref[:, i * 256:(i + 1) * 256] = ag2_buf[i]
    sent = (
        part_rx, rs_tx, ss_buf.at[pl.ds(0, 15)], ag_buf.at[pl.ds(0, 15)], act_buf.at[0],
        rs2_tx, ag2_buf.at[pl.ds(0, 15)], qkv_buf.at[0],
    )
    for phase, ref in enumerate(sent):
        wait_bytes(ref, send_sem.at[phase])


def store_kernel(
    pos, x2_ref, kn_ref, vn_ref, k_in, v_in, out_ref, k_out, v_out, k_buf, v_buf, x2, x_sem, k_sem, v_sem
):
    rows, keys = k_out.shape[:2]
    x2[...] = x2_ref[...].astype(BF16)
    out = pltpu.make_async_copy(x2, out_ref, x_sem)
    out.start()
    first_slot = lax.axis_index("sp") * (keys // 2)
    row16 = lax.broadcasted_iota(jnp.int32, (16, 128), 0)

    def put(ref, new, b, ploc):
        start = pl.multiple_of((jnp.clip(ploc * 2, 0, keys - 2) // 16) * 16, 16)
        block = ref[b, pl.ds(start, 16), :].astype(F32)
        at = row16 + start
        block = jnp.where(at == ploc * 2, new[0, b:b + 1, :], block)
        block = jnp.where(at == ploc * 2 + 1, new[1, b:b + 1, :], block)
        ref[b, pl.ds(start, 16), :] = block.astype(BF16)

    for b in range(rows):
        ploc = pos[b] - first_slot
        put(k_buf, kn_ref, b, ploc)
        pltpu.make_async_copy(k_buf.at[b], k_out.at[b], k_sem).start()
        put(v_buf, vn_ref, b, ploc)
        pltpu.make_async_copy(v_buf.at[b], v_out.at[b], v_sem).start()
    out.wait()
    pltpu.make_async_copy(k_buf, k_out, k_sem).wait()
    pltpu.make_async_copy(v_buf, v_out, v_sem).wait()


def solution(mesh):
    cache_spec = P("dp", "sp", "tp", None)
    vmem = pl.BlockSpec(memory_space=pltpu.VMEM)
    smem = pl.BlockSpec(memory_space=pltpu.SMEM)
    hbm = pl.BlockSpec(memory_space=pltpu.HBM)

    def in_hbm(*arrays):
        return tuple(pltpu.with_memory_space_constraint(a, pltpu.HBM) for a in arrays)

    def local_step(hidden, positions, norm_attn, norm_mlp, w_qkv, w_out, w_gate_up, w_down, k_cache, v_cache):
        rows, block_len, kv_local, head_dim = k_cache.shape
        dim = hidden.shape[1]
        flat = (rows, block_len * kv_local, head_dim)
        freq = ROPE_BASE ** (-np.arange(0, head_dim, 2, dtype=np.float64) / head_dim)
        freq = jnp.asarray(np.concatenate([freq, freq])[None].astype(np.float32))
        units = w_down.shape[0] // 2
        fresh = (kv_local, rows, head_dim)
        x2, k_mid, v_mid, k_new, v_new, pos = pl.pallas_call(
            layer_kernel,
            out_shape=(
                pltpu.VMEM((rows, dim), F32),
                pltpu.VMEM(flat, BF16),
                pltpu.VMEM(flat, BF16),
                pltpu.VMEM(fresh, F32),
                pltpu.VMEM(fresh, F32),
                pltpu.SMEM((rows,), jnp.int32),
            ),
            in_specs=[hbm] * 11,
            out_specs=(vmem,) * 5 + (smem,),
            scratch_shapes=[
                pltpu.VMEM((1, head_dim), F32),
                pltpu.VMEM((rows, dim), BF16),
                pltpu.VMEM((1, dim), F32),
                pltpu.VMEM((1, dim), F32),
                pltpu.VMEM((TP, 1024, 256), BF16),
                pltpu.VMEM((dim, 2 * units), BF16),
                pltpu.VMEM((2, units, 1024), BF16),
                pltpu.VMEM((rows, dim), BF16),
                pltpu.VMEM((2, rows, w_qkv.shape[1] // 2), F32),
                pltpu.VMEM((rows, 8, 128), F32),
                pltpu.VMEM((rows + 2, 8, 128), F32),
                pltpu.VMEM((3, rows + 2, 8, 128), F32),
                pltpu.VMEM((rows, 8, 128), F32),
                pltpu.VMEM((rows, 1024), BF16),
                pltpu.VMEM((TP, rows, 256), F32),
                pltpu.VMEM((TP, rows, 256), F32),
                pltpu.VMEM((16, rows, 256), F32),
                pltpu.VMEM((16, 1, 128), F32),
                pltpu.VMEM((2, rows, units), F32),
                pltpu.VMEM((TP, rows, 256), F32),
                pltpu.VMEM((TP, rows, 256), F32),
                pltpu.VMEM((TP, rows, 256), F32),
                pltpu.VMEM((16, rows, 256), F32),
                pltpu.SemaphoreType.DMA((5,)),
                pltpu.SemaphoreType.DMA((W_CHUNKS,)),
                pltpu.SemaphoreType.DMA((rows // GROUP,)),
                pltpu.SemaphoreType.DMA((rows // GROUP,)),
                pltpu.SemaphoreType.DMA,
                pltpu.SemaphoreType.DMA,
                pltpu.SemaphoreType.DMA,
                pltpu.SemaphoreType.DMA((rows // GROUP + 2,)),
                pltpu.SemaphoreType.DMA,
                pltpu.SemaphoreType.DMA,
                pltpu.SemaphoreType.DMA((10,)),
                pltpu.SemaphoreType.DMA,
                pltpu.SemaphoreType.DMA,
                pltpu.SemaphoreType.DMA((10,)),
                pltpu.SemaphoreType.DMA,
                pltpu.SemaphoreType.DMA((8,)),
            ],
            compiler_params=pltpu.CompilerParams(
                collective_id=0, has_side_effects=True, vmem_limit_bytes=44 * 2 ** 20
            ),
            cost_estimate=pl.CostEstimate(flops=4 * 10 ** 9, bytes_accessed=6 * 10 ** 7, transcendentals=10 ** 6),
        )(*in_hbm(
            positions, freq, hidden, norm_attn.reshape(1, dim), norm_mlp.reshape(1, dim), w_qkv,
            k_cache.reshape(flat), v_cache.reshape(flat), w_out, w_gate_up, w_down,
        ))
        result, k_upd, v_upd, _, _ = pl.pallas_call(
            store_kernel,
            out_shape=(
                jax.ShapeDtypeStruct((rows, dim), BF16),
                jax.ShapeDtypeStruct(flat, BF16),
                jax.ShapeDtypeStruct(flat, BF16),
                pltpu.VMEM(flat, BF16),
                pltpu.VMEM(flat, BF16),
            ),
            in_specs=[smem] + [vmem] * 5,
            out_specs=(hbm, hbm, hbm, vmem, vmem),
            input_output_aliases={4: 3, 5: 4},
            scratch_shapes=[
                pltpu.VMEM((rows, dim), BF16),
                pltpu.SemaphoreType.DMA,
                pltpu.SemaphoreType.DMA,
                pltpu.SemaphoreType.DMA,
            ],
            compiler_params=pltpu.CompilerParams(vmem_limit_bytes=8 * 2 ** 20),
            cost_estimate=pl.CostEstimate(flops=10 ** 8, bytes_accessed=2 * 10 ** 7, transcendentals=0),
        )(pos, x2, k_new, v_new, k_mid, v_mid)
        return result, k_upd.reshape(k_cache.shape), v_upd.reshape(v_cache.shape)

    return jax.shard_map(
        local_step, mesh=mesh,
        in_specs=(P("dp", None), P("dp"), P(None), P(None), P(None, "tp"), P("tp", None), P(None, "tp"), P("tp", None), cache_spec, cache_spec),
        out_specs=(P("dp", None), cache_spec, cache_spec), check_vma=False,
    )
```

```python
import jax
import jax.numpy as jnp
import numpy as np
from jax import lax
from jax.experimental import pallas as pl
from jax.experimental.pallas import tpu as pltpu
from jax.sharding import PartitionSpec as P

WINDOW = 2047
ROPE_BASE = 10000.0
NORM_EPS = 1e-5
MESH = pl.DeviceIdType.MESH
F32 = jnp.float32
BF16 = jnp.bfloat16
NEG = float(jnp.finfo(jnp.float32).min)

TP = 4
SP = 4
W_CHUNKS = 4
GROUP = 2
FLIGHT = 3
OFFSETS = (
    (0, 1), (0, 3), (1, 1), (2, 1), (1, 3), (3, 1), (2, 3), (3, 3),
    (0, 2), (1, 0), (2, 0), (1, 2), (3, 0), (2, 2), (3, 2),
)
VIA = {off: off if off[1] & 1 else (0, 1) for off in OFFSETS}


def add_offsets(a, b):
    return (a[0] ^ b[0], a[1] ^ b[1])


def layer_kernel(
    pos_ref, freq_ref, x_ref, gain_ref, gain2_ref, wq_ref, k_ref, v_ref, wo_ref, wg_ref, wd_ref,
    out_ref, k_buf, v_buf, kn_buf, vn_buf, pos,
    freq, x_buf, gain, gain2, wo_buf, wg_buf, wd_buf,
    r_buf, qkv_buf, q_buf, part, part_rx, o_buf, ob_buf, rs_tx, rs_rx, ag_buf, ss_buf,
    act_a, act_b, dn_buf, rs2_tx, rs2_rx, ag2_buf,
    in_sem, wq_sem, k_sem, wo_sem, wg_sem, wd_sem,
    a_sem, b_sem, s_sem, g_sem, c_sem, d_sem, e_sem, q_sem, send_sem,
):
    dp, t, s = lax.axis_index("dp"), lax.axis_index("tp"), lax.axis_index("sp")
    rows, dim = x_ref.shape
    keys = k_ref.shape[1]
    units = wg_buf.shape[1] // 2
    ffn = wd_ref.shape[0]
    depth = dim // W_CHUNKS
    core = s & 1
    q_cols = wq_ref.shape[1] // 2
    wq_buf = wg_buf.at[:, pl.ds(0, q_cols)]

    def peer(off):
        return (dp, t ^ off[0], s ^ off[1])

    def piece_of(off):
        return (s ^ off[1] ^ 1) * TP + (t ^ off[0])

    me = piece_of((0, 0))

    def remote(src, dst, phase, recv, off):
        return pltpu.make_async_remote_copy(
            src_ref=src, dst_ref=dst, send_sem=send_sem.at[phase], recv_sem=recv,
            device_id=peer(off), device_id_type=MESH,
        )

    def wait_bytes(ref, sem):
        pltpu.make_async_copy(ref, ref, sem).wait()

    small = [
        pltpu.make_async_copy(src, dst, in_sem.at[i])
        for i, (src, dst) in enumerate((
            (x_ref, x_buf), (gain_ref, gain), (freq_ref, freq), (pos_ref, pos), (gain2_ref, gain2)
        ))
    ]
    for copy in small:
        copy.start()

    def wq_copy(c):
        at = pl.ds(c * depth, depth)
        cols = pl.ds(pl.multiple_of(core * q_cols, 128), q_cols)
        return pltpu.make_async_copy(wq_ref.at[at, cols], wq_buf.at[at], wq_sem.at[c])

    def k_copy(g):
        at = pl.ds(g * GROUP, GROUP)
        return pltpu.make_async_copy(k_ref.at[at], k_buf.at[at], k_sem.at[g])

    def v_copy(g):
        at = pl.ds(g * GROUP, GROUP)
        return pltpu.make_async_copy(v_ref.at[at], v_buf.at[at], k_sem.at[g])

    def start_wo():
        for d in range(TP):
            col = pl.multiple_of((s * TP + d) * 256, 256)
            pltpu.make_async_copy(wo_ref.at[:, pl.ds(col, 256)], wo_buf.at[d], wo_sem).start()

    def start_wg(c):
        for half in range(2):
            col = pl.multiple_of(half * ffn + core * units, 128)
            pltpu.make_async_copy(
                wg_ref.at[pl.ds(c * 1024, 1024), pl.ds(col, units)],
                wg_buf.at[pl.ds(c * 1024, 1024), pl.ds(half * units, units)],
                wg_sem,
            ).start()

    def start_wd():
        for c in range(2):
            col = pl.multiple_of(s * 1024, 1024)
            pltpu.make_async_copy(
                wd_ref.at[pl.ds(c * units, units), pl.ds(col, 1024)], wd_buf.at[c], wd_sem
            ).start()

    def kv_loads(g):
        return [k_copy(g), v_copy(g)]

    loads = [[wq_copy(c)] for c in range(W_CHUNKS)] + [kv_loads(g) for g in range(rows // GROUP)]

    def start_load(i):
        if i < len(loads):
            for copy in loads[i]:
                copy.start()

    for i in range(FLIGHT):
        start_load(i)
    barrier = pltpu.get_barrier_semaphore()
    for off in OFFSETS:
        pl.semaphore_signal(barrier, inc=1, device_id=peer(off), device_id_type=MESH)

    wq_copy(0).wait()
    start_load(FLIGHT)
    for copy in small:
        copy.wait()
    x = x_buf[...].astype(F32)
    scale = lax.rsqrt(jnp.mean(x * x, axis=-1, keepdims=True) + NORM_EPS)
    r_buf[...] = (x * scale * gain[...]).astype(BF16)
    row_id = lax.broadcasted_iota(jnp.int32, (rows, 128), 0)
    lane_id = lax.broadcasted_iota(jnp.int32, (rows, 128), 1)
    diag = row_id == lane_id

    def qkv_term(c):
        at = pl.ds(c * depth, depth)
        return jnp.dot(r_buf[:, c * depth:(c + 1) * depth], wq_buf[at, :], preferred_element_type=F32)

    qkv = qkv_term(0)
    pos_col = jnp.zeros((rows, 128), jnp.int32)
    for b in range(rows):
        pos_col = jnp.where(row_id == b, pos[b], pos_col)
    angle = pos_col.astype(F32) * freq[...]
    cos = jnp.cos(angle)
    sin = jnp.sin(angle)
    sin = jnp.where(lane_id < 64, -sin, sin)
    for c in range(1, W_CHUNKS):
        wq_copy(c).wait()
        start_load(FLIGHT + c)
        if c == W_CHUNKS - 1:
            start_load(FLIGHT + c + 1)
            start_load(FLIGHT + c + 2)
        qkv = qkv + qkv_term(c)

    qkv_buf[core] = qkv
    pl.semaphore_wait(barrier, len(OFFSETS))
    remote(qkv_buf.at[core], qkv_buf.at[core], 7, q_sem, (0, 1)).start()
    wait_bytes(qkv_buf.at[1 - core], q_sem)
    def rotate(vals):
        out = vals * cos + pltpu.roll(vals, 64, 1) * sin
        return out.astype(BF16).astype(F32)

    for kv in range(2):
        for h in range(4):
            q_buf[:, kv * 4 + h, :] = rotate(qkv_buf[kv, :, h * 128:(h + 1) * 128])
        kn_buf[kv] = rotate(qkv_buf[kv, :, 512:640])
        vn_buf[kv] = qkv_buf[kv, :, 640:768].astype(BF16).astype(F32)

    first_slot = s * (keys // 2)
    lane = lax.broadcasted_iota(jnp.int32, (8, keys), 1)
    head = lax.broadcasted_iota(jnp.int32, (8, keys), 0)
    own = (lane & 1) == (head >> 2)
    slot_id = lane >> 1
    lane8 = lax.broadcasted_iota(jnp.int32, (8, 128), 1)
    sub8 = lax.broadcasted_iota(jnp.int32, (8, 128), 0)
    low_heads = sub8 < 4
    scale = 128 ** -0.5

    def new_rows(buf, b):
        return jnp.where(low_heads, buf[0, pl.ds(b, 1), :], buf[1, pl.ds(b, 1), :])

    def a_rows(g):
        return pl.ds(g * GROUP, GROUP + (2 if g == rows // GROUP - 1 else 0))

    groups = rows // GROUP

    def a_start(g, k):
        remote(part.at[a_rows(g)], part_rx.at[k, a_rows(g)], 0, a_sem.at[k], (0, k + 1)).start()

    m_all = jnp.zeros((8, 128), F32)
    l_all = jnp.zeros((8, 128), F32)
    n_all = jnp.zeros((8, 128), F32)

    def group_scores(g):
        wait_bytes(k_buf.at[pl.ds(0, 2 * GROUP)], k_sem.at[g])
        start_load(W_CHUNKS + FLIGHT + 2 + g)
        return [
            lax.dot_general(
                q_buf[b].astype(BF16), k_buf[b], (((1,), (1,)), ((), ())), preferred_element_type=F32
            )
            for b in range(g * GROUP, (g + 1) * GROUP)
        ]

    pending = group_scores(0)
    for g in range(groups):
        ids = range(g * GROUP, (g + 1) * GROUP)
        scores = pending
        if g + 1 < groups:
            pending = group_scores(g + 1)
        probs = []
        for b, sc in zip(ids, scores):
            fresh = jnp.sum(q_buf[b] * new_rows(kn_buf, b), axis=-1, keepdims=True) * scale
            ploc = pos[b] - first_slot
            mask = own & (slot_id < ploc) & (slot_id >= ploc - WINDOW)
            sc = jnp.where(mask, sc * scale, NEG)
            m = jnp.max(sc, axis=-1, keepdims=True)
            w = jnp.where(mask, jnp.exp(sc - m), 0.0)
            l = jnp.sum(w, axis=-1, keepdims=True)
            at = lane8 == sub8 + b * 8
            n_all = jnp.where(at, fresh, n_all)
            m_all = jnp.where(at, m, m_all)
            l_all = jnp.where(at, l, l_all)
            probs.append(w.astype(BF16))
        for b, w in zip(ids, probs):
            part[b] = jnp.dot(w, v_buf[b], preferred_element_type=F32)
        if g == rows // GROUP - 1:
            part[rows] = m_all
            part[rows + 1] = l_all
        for k in (1, 2, 0):
            a_start(g, k)
        if g == groups - 2:
            start_wo()
    for c in range(4):
        start_wg(c)
    start_wd()

    for k in range(3):
        wait_bytes(part_rx.at[k], a_sem.at[k])
    parts = [part, part_rx.at[0], part_rx.at[1], part_rx.at[2]]
    top = n_all
    for p in parts:
        top = jnp.maximum(top, p[rows])
    facs = [jnp.exp(p[rows] - top) for p in parts]
    fresh = jnp.exp(n_all - top)
    total = fresh
    for p, f in zip(parts, facs):
        total = total + p[rows + 1] * f
    inv = 1.0 / total
    facs = [f * inv for f in facs]
    fresh = fresh * inv
    for b in range(rows):
        at = lane8 == sub8 + b * 8
        o = new_rows(vn_buf, b) * jnp.sum(jnp.where(at, fresh, 0.0), axis=-1, keepdims=True)
        for p, f in zip(parts, facs):
            o = o + p[b] * jnp.sum(jnp.where(at, f, 0.0), axis=-1, keepdims=True)
        o_buf[b] = o
    for h in range(8):
        ob_buf[:, h * 128:(h + 1) * 128] = o_buf[:, h, :].astype(BF16)

    def reduce_scatter(make_term, tx, rx, phase, sem):
        for dts in ((3,), (2, 1, 0)):
            for dt in dts:
                tx[dt] = make_term(t ^ dt)
            for dt in dts:
                remote(tx.at[dt], rx.at[dt], phase, sem, (dt, 1)).start()
        wait_bytes(rx, sem)
        return rx[0] + rx[1] + rx[2] + rx[3]

    wait_bytes(wo_buf, wo_sem)
    o_all = ob_buf[...]

    def out_term(d):
        return jnp.dot(o_all, wo_buf[d], preferred_element_type=F32).astype(BF16).astype(F32)

    my_cols = pl.ds(pl.multiple_of(me * 256, 256), 256)
    mid = x_buf[:, my_cols].astype(F32) + reduce_scatter(out_term, rs_tx, rs_rx, 1, b_sem)
    ag_buf[me] = mid
    sq = jnp.sum(mid * mid, axis=-1, keepdims=True)
    ss_buf[me] = jnp.sum(jnp.where(diag, sq, 0.0), axis=0, keepdims=True)

    class Gather:
        def __init__(self, buf, sems, phase):
            self.buf, self.sems, self.phase = buf, sems, phase

        def send(self, have):
            for k in reversed(range(len(OFFSETS))):
                off = OFFSETS[k]
                if add_offsets(off, VIA[off]) == have:
                    slot = piece_of(have)
                    recv = self.sems.at[k if k < 8 else 8 + off[1] // 2]
                    remote(self.buf.at[slot], self.buf.at[slot], self.phase, recv, VIA[off]).start()

        def wait(self, off):
            slot = piece_of(off)
            k = OFFSETS.index(off)
            remote(self.buf.at[slot], self.buf.at[slot], self.phase, self.sems.at[k], off).wait_recv()
            self.send(off)

        def wait_block(self, ds):
            wait_bytes(self.buf.at[pl.ds(0, 3 if ds == 0 else 4)], self.sems.at[8 + ds // 2])

    for off in sorted(OFFSETS, key=lambda o: -o[0]):
        remote(ss_buf.at[me], ss_buf.at[me], 2, s_sem, off).start()
    gather = Gather(ag_buf, g_sem, 3)
    gather.send((0, 0))
    for off in OFFSETS[:3]:
        gather.wait(off)
    wait_bytes(ss_buf.at[pl.ds(0, len(OFFSETS))], s_sem)
    tot = jnp.sum(ss_buf[...], axis=0)
    mean_sq = jnp.sum(jnp.where(diag, tot, 0.0), axis=-1, keepdims=True) / dim
    rstd = lax.rsqrt(mean_sq + NORM_EPS)
    wait_bytes(wg_buf, wg_sem)

    def normed(off):
        slot = piece_of(off)
        at = pl.ds(pl.multiple_of(slot * 256, 256), 256)
        return (ag_buf[slot] * rstd * gain2[:, at]).astype(BF16), at

    def gate_up(pieces, cols):
        out = None
        for r2, at in pieces:
            term = jnp.dot(r2, wg_buf[at, cols], preferred_element_type=F32)
            out = term if out is None else out + term
        return out

    whole = slice(0, 2 * units)
    hid = gate_up([normed(off) for off in ((0, 0),) + OFFSETS[:3]], whole)
    for off in OFFSETS[3:8]:
        gather.wait(off)
    hid = hid + gate_up([normed(off) for off in OFFSETS[3:8]], whole)
    gather.wait_block(0)
    gather.wait_block(2)
    late = [normed(off) for off in OFFSETS[8:]]
    acts = (act_a, act_b)
    spans = (slice(0, act_a.shape[2]), slice(act_a.shape[2], units))
    for i in range(2):
        g_cols = spans[i]
        u_cols = slice(units + g_cols.start, units + g_cols.stop)
        gate = hid[:, g_cols] + gate_up(late, g_cols)
        up = hid[:, u_cols] + gate_up(late, u_cols)
        acts[i][core] = (gate * jax.nn.sigmoid(gate) * up).astype(BF16).astype(F32)
        remote(acts[i].at[core], acts[i].at[core], 4 + 4 * i, c_sem.at[i], (0, 1)).start()

    wait_bytes(wd_buf, wd_sem)

    def down_part(i, which):
        return jnp.dot(acts[i][which].astype(BF16), wd_buf[which, spans[i], :], preferred_element_type=F32)

    down = down_part(0, core) + down_part(1, core)
    for i in range(2):
        wait_bytes(acts[i].at[1 - core], c_sem.at[i])
        down = down + down_part(i, 1 - core)
    down = down.astype(BF16).astype(F32)
    for d in range(TP):
        dn_buf[d] = down[:, d * 256:(d + 1) * 256]

    def down_term(d):
        return dn_buf[d]

    ag2_buf[me] = mid + reduce_scatter(down_term, rs2_tx, rs2_rx, 5, d_sem)
    gather2 = Gather(ag2_buf, e_sem, 6)
    gather2.send((0, 0))
    for off in OFFSETS[:8]:
        gather2.wait(off)
    gather2.wait_block(0)
    gather2.wait_block(2)
    for i in range(16):
        out_ref[:, i * 256:(i + 1) * 256] = ag2_buf[i]
    sent = (
        part_rx, rs_tx, ss_buf.at[pl.ds(0, 15)], ag_buf.at[pl.ds(0, 15)], act_a.at[0],
        rs2_tx, ag2_buf.at[pl.ds(0, 15)], qkv_buf.at[0], act_b.at[0],
    )
    for phase, ref in enumerate(sent):
        wait_bytes(ref, send_sem.at[phase])


def store_kernel(
    pos, x2_ref, kn_ref, vn_ref, k_in, v_in, out_ref, k_out, v_out, k_buf, v_buf, x2, x_sem, k_sem, v_sem
):
    rows, keys = k_out.shape[:2]
    x2[...] = x2_ref[...].astype(BF16)
    out = pltpu.make_async_copy(x2, out_ref, x_sem)
    out.start()
    first_slot = lax.axis_index("sp") * (keys // 2)
    row16 = lax.broadcasted_iota(jnp.int32, (16, 128), 0)

    def put(ref, new, b, ploc):
        start = pl.multiple_of((jnp.clip(ploc * 2, 0, keys - 2) // 16) * 16, 16)
        block = ref[b, pl.ds(start, 16), :].astype(F32)
        at = row16 + start
        block = jnp.where(at == ploc * 2, new[0, b:b + 1, :], block)
        block = jnp.where(at == ploc * 2 + 1, new[1, b:b + 1, :], block)
        ref[b, pl.ds(start, 16), :] = block.astype(BF16)

    for b in range(rows):
        ploc = pos[b] - first_slot
        put(k_buf, kn_ref, b, ploc)
        pltpu.make_async_copy(k_buf.at[b], k_out.at[b], k_sem).start()
        put(v_buf, vn_ref, b, ploc)
        pltpu.make_async_copy(v_buf.at[b], v_out.at[b], v_sem).start()
    out.wait()
    pltpu.make_async_copy(k_buf, k_out, k_sem).wait()
    pltpu.make_async_copy(v_buf, v_out, v_sem).wait()


def solution(mesh):
    cache_spec = P("dp", "sp", "tp", None)
    vmem = pl.BlockSpec(memory_space=pltpu.VMEM)
    smem = pl.BlockSpec(memory_space=pltpu.SMEM)
    hbm = pl.BlockSpec(memory_space=pltpu.HBM)

    def in_hbm(*arrays):
        return tuple(pltpu.with_memory_space_constraint(a, pltpu.HBM) for a in arrays)

    def local_step(hidden, positions, norm_attn, norm_mlp, w_qkv, w_out, w_gate_up, w_down, k_cache, v_cache):
        rows, block_len, kv_local, head_dim = k_cache.shape
        dim = hidden.shape[1]
        flat = (rows, block_len * kv_local, head_dim)
        freq = ROPE_BASE ** (-np.arange(0, head_dim, 2, dtype=np.float64) / head_dim)
        freq = jnp.asarray(np.concatenate([freq, freq])[None].astype(np.float32))
        units = w_down.shape[0] // 2
        fresh = (kv_local, rows, head_dim)
        x2, k_mid, v_mid, k_new, v_new, pos = pl.pallas_call(
            layer_kernel,
            out_shape=(
                pltpu.VMEM((rows, dim), F32),
                pltpu.VMEM(flat, BF16),
                pltpu.VMEM(flat, BF16),
                pltpu.VMEM(fresh, F32),
                pltpu.VMEM(fresh, F32),
                pltpu.SMEM((rows,), jnp.int32),
            ),
            in_specs=[hbm] * 11,
            out_specs=(vmem,) * 5 + (smem,),
            scratch_shapes=[
                pltpu.VMEM((1, head_dim), F32),
                pltpu.VMEM((rows, dim), BF16),
                pltpu.VMEM((1, dim), F32),
                pltpu.VMEM((1, dim), F32),
                pltpu.VMEM((TP, 1024, 256), BF16),
                pltpu.VMEM((dim, 2 * units), BF16),
                pltpu.VMEM((2, units, 1024), BF16),
                pltpu.VMEM((rows, dim), BF16),
                pltpu.VMEM((2, rows, w_qkv.shape[1] // 2), F32),
                pltpu.VMEM((rows, 8, 128), F32),
                pltpu.VMEM((rows + 2, 8, 128), F32),
                pltpu.VMEM((3, rows + 2, 8, 128), F32),
                pltpu.VMEM((rows, 8, 128), F32),
                pltpu.VMEM((rows, 1024), BF16),
                pltpu.VMEM((TP, rows, 256), F32),
                pltpu.VMEM((TP, rows, 256), F32),
                pltpu.VMEM((16, rows, 256), F32),
                pltpu.VMEM((16, 1, 128), F32),
                pltpu.VMEM((2, rows, 1024), F32),
                pltpu.VMEM((2, rows, units - 1024), F32),
                pltpu.VMEM((TP, rows, 256), F32),
                pltpu.VMEM((TP, rows, 256), F32),
                pltpu.VMEM((TP, rows, 256), F32),
                pltpu.VMEM((16, rows, 256), F32),
                pltpu.SemaphoreType.DMA((5,)),
                pltpu.SemaphoreType.DMA((W_CHUNKS,)),
                pltpu.SemaphoreType.DMA((rows // GROUP,)),
                pltpu.SemaphoreType.DMA,
                pltpu.SemaphoreType.DMA,
                pltpu.SemaphoreType.DMA,
                pltpu.SemaphoreType.DMA((3,)),
                pltpu.SemaphoreType.DMA,
                pltpu.SemaphoreType.DMA,
                pltpu.SemaphoreType.DMA((10,)),
                pltpu.SemaphoreType.DMA((2,)),
                pltpu.SemaphoreType.DMA,
                pltpu.SemaphoreType.DMA((10,)),
                pltpu.SemaphoreType.DMA,
                pltpu.SemaphoreType.DMA((9,)),
            ],
            compiler_params=pltpu.CompilerParams(
                collective_id=0, has_side_effects=True, vmem_limit_bytes=44 * 2 ** 20
            ),
            cost_estimate=pl.CostEstimate(flops=4 * 10 ** 9, bytes_accessed=6 * 10 ** 7, transcendentals=10 ** 6),
        )(*in_hbm(
            positions, freq, hidden, norm_attn.reshape(1, dim), norm_mlp.reshape(1, dim), w_qkv,
            k_cache.reshape(flat), v_cache.reshape(flat), w_out, w_gate_up, w_down,
        ))
        result, k_upd, v_upd, _, _ = pl.pallas_call(
            store_kernel,
            out_shape=(
                jax.ShapeDtypeStruct((rows, dim), BF16),
                jax.ShapeDtypeStruct(flat, BF16),
                jax.ShapeDtypeStruct(flat, BF16),
                pltpu.VMEM(flat, BF16),
                pltpu.VMEM(flat, BF16),
            ),
            in_specs=[smem] + [vmem] * 5,
            out_specs=(hbm, hbm, hbm, vmem, vmem),
            input_output_aliases={4: 3, 5: 4},
            scratch_shapes=[
                pltpu.VMEM((rows, dim), BF16),
                pltpu.SemaphoreType.DMA,
                pltpu.SemaphoreType.DMA,
                pltpu.SemaphoreType.DMA,
            ],
            compiler_params=pltpu.CompilerParams(vmem_limit_bytes=8 * 2 ** 20),
            cost_estimate=pl.CostEstimate(flops=10 ** 8, bytes_accessed=2 * 10 ** 7, transcendentals=0),
        )(pos, x2, k_new, v_new, k_mid, v_mid)
        return result, k_upd.reshape(k_cache.shape), v_upd.reshape(v_cache.shape)

    return jax.shard_map(
        local_step, mesh=mesh,
        in_specs=(P("dp", None), P("dp"), P(None), P(None), P(None, "tp"), P("tp", None), P(None, "tp"), P("tp", None), cache_spec, cache_spec),
        out_specs=(P("dp", None), cache_spec, cache_spec), check_vma=False,
    )
```

```python
import jax
import jax.numpy as jnp
import numpy as np
from jax import lax
from jax.experimental import pallas as pl
from jax.experimental.pallas import tpu as pltpu
from jax.sharding import PartitionSpec as P

WINDOW = 2047
ROPE_BASE = 10000.0
NORM_EPS = 1e-5
MESH = pl.DeviceIdType.MESH
F32 = jnp.float32
BF16 = jnp.bfloat16
NEG = float(jnp.finfo(jnp.float32).min)

TP = 4
SP = 4
W_CHUNKS = 4
GROUP = 2
FLIGHT = 3
OFFSETS = (
    (0, 1), (0, 3), (1, 1), (2, 1), (1, 3), (3, 1), (2, 3), (3, 3),
    (0, 2), (1, 0), (2, 0), (1, 2), (3, 0), (2, 2), (3, 2),
)
VIA = {off: off if off[1] & 1 else (0, 1) for off in OFFSETS}


def add_offsets(a, b):
    return (a[0] ^ b[0], a[1] ^ b[1])


def layer_kernel(
    pos_ref, freq_ref, x_ref, gain_ref, gain2_ref, wq_ref, k_ref, v_ref, wo_ref, wg_ref, wd_ref,
    out_ref, k_buf, v_buf, kn_buf, vn_buf, pos,
    freq, x_buf, gain, gain2, wo_buf, wg_buf, wd_buf,
    r_buf, qkv_buf, q_buf, part, part_rx, o_buf, ob_buf, rs_tx, rs_rx, ag_buf, ss_buf,
    act_a, act_b, dn_buf, rs2_rx, ag2_buf,
    in_sem, wq_sem, k_sem, wo_sem, wg_sem, wd_sem,
    a_sem, b_sem, s_sem, g_sem, c_sem, d_sem, e_sem, q_sem, send_sem,
):
    dp, t, s = lax.axis_index("dp"), lax.axis_index("tp"), lax.axis_index("sp")
    rows, dim = x_ref.shape
    keys = k_ref.shape[1]
    units = wg_buf.shape[1] // 2
    ffn = wd_ref.shape[0]
    depth = dim // W_CHUNKS
    core = s & 1
    q_cols = wq_ref.shape[1] // 2
    wq_buf = wg_buf.at[:, pl.ds(0, q_cols)]

    def peer(off):
        return (dp, t ^ off[0], s ^ off[1])

    def piece_of(off):
        return (s ^ off[1] ^ 1) * TP + (t ^ off[0])

    me = piece_of((0, 0))

    def remote(src, dst, phase, recv, off):
        return pltpu.make_async_remote_copy(
            src_ref=src, dst_ref=dst, send_sem=send_sem.at[phase], recv_sem=recv,
            device_id=peer(off), device_id_type=MESH,
        )

    def wait_bytes(ref, sem):
        pltpu.make_async_copy(ref, ref, sem).wait()

    small = [
        pltpu.make_async_copy(src, dst, in_sem.at[i])
        for i, (src, dst) in enumerate((
            (x_ref, x_buf), (gain_ref, gain), (freq_ref, freq), (pos_ref, pos), (gain2_ref, gain2)
        ))
    ]
    for copy in small:
        copy.start()

    def wq_copy(c):
        at = pl.ds(c * depth, depth)
        cols = pl.ds(pl.multiple_of(core * q_cols, 128), q_cols)
        return pltpu.make_async_copy(wq_ref.at[at, cols], wq_buf.at[at], wq_sem.at[c])

    def k_copy(g):
        at = pl.ds(g * GROUP, GROUP)
        return pltpu.make_async_copy(k_ref.at[at], k_buf.at[at], k_sem.at[g])

    def v_copy(g):
        at = pl.ds(g * GROUP, GROUP)
        return pltpu.make_async_copy(v_ref.at[at], v_buf.at[at], k_sem.at[g])

    def start_wo():
        for d in range(TP):
            col = pl.multiple_of((s * TP + d) * 256, 256)
            pltpu.make_async_copy(wo_ref.at[:, pl.ds(col, 256)], wo_buf.at[d], wo_sem).start()

    def start_wg(c):
        for half in range(2):
            col = pl.multiple_of(half * ffn + core * units, 128)
            pltpu.make_async_copy(
                wg_ref.at[pl.ds(c * 1024, 1024), pl.ds(col, units)],
                wg_buf.at[pl.ds(c * 1024, 1024), pl.ds(half * units, units)],
                wg_sem,
            ).start()

    def start_wd():
        for c in range(2):
            col = pl.multiple_of(s * 1024, 1024)
            pltpu.make_async_copy(
                wd_ref.at[pl.ds(c * units, units), pl.ds(col, 1024)], wd_buf.at[c], wd_sem
            ).start()

    def kv_loads(g):
        return [k_copy(g), v_copy(g)]

    loads = [[wq_copy(c)] for c in range(W_CHUNKS)] + [kv_loads(g) for g in range(rows // GROUP)]

    def start_load(i):
        if i < len(loads):
            for copy in loads[i]:
                copy.start()

    for i in range(FLIGHT):
        start_load(i)
    barrier = pltpu.get_barrier_semaphore()
    for off in OFFSETS:
        pl.semaphore_signal(barrier, inc=1, device_id=peer(off), device_id_type=MESH)

    wq_copy(0).wait()
    start_load(FLIGHT)
    for copy in small:
        copy.wait()
    x = x_buf[...].astype(F32)
    scale = lax.rsqrt(jnp.mean(x * x, axis=-1, keepdims=True) + NORM_EPS)
    r_buf[...] = (x * scale * gain[...]).astype(BF16)
    row_id = lax.broadcasted_iota(jnp.int32, (rows, 128), 0)
    lane_id = lax.broadcasted_iota(jnp.int32, (rows, 128), 1)
    diag = row_id == lane_id

    def qkv_term(c):
        at = pl.ds(c * depth, depth)
        return jnp.dot(r_buf[:, c * depth:(c + 1) * depth], wq_buf[at, :], preferred_element_type=F32)

    qkv = qkv_term(0)
    pos_col = jnp.zeros((rows, 128), jnp.int32)
    for b in range(rows):
        pos_col = jnp.where(row_id == b, pos[b], pos_col)
    angle = pos_col.astype(F32) * freq[...]
    cos = jnp.cos(angle)
    sin = jnp.sin(angle)
    sin = jnp.where(lane_id < 64, -sin, sin)
    for c in range(1, W_CHUNKS):
        wq_copy(c).wait()
        start_load(FLIGHT + c)
        if c == W_CHUNKS - 1:
            start_load(FLIGHT + c + 1)
            start_load(FLIGHT + c + 2)
        qkv = qkv + qkv_term(c)

    qkv_buf[core] = qkv
    pl.semaphore_wait(barrier, len(OFFSETS))
    remote(qkv_buf.at[core], qkv_buf.at[core], 7, q_sem, (0, 1)).start()
    wait_bytes(qkv_buf.at[1 - core], q_sem)
    def rotate(vals):
        out = vals * cos + pltpu.roll(vals, 64, 1) * sin
        return out.astype(BF16).astype(F32)

    for kv in range(2):
        for h in range(4):
            q_buf[:, kv * 4 + h, :] = rotate(qkv_buf[kv, :, h * 128:(h + 1) * 128])
        kn_buf[kv] = rotate(qkv_buf[kv, :, 512:640])
        vn_buf[kv] = qkv_buf[kv, :, 640:768].astype(BF16).astype(F32)

    first_slot = s * (keys // 2)
    lane = lax.broadcasted_iota(jnp.int32, (8, keys), 1)
    head = lax.broadcasted_iota(jnp.int32, (8, keys), 0)
    own = (lane & 1) == (head >> 2)
    slot_id = lane >> 1
    lane8 = lax.broadcasted_iota(jnp.int32, (8, 128), 1)
    sub8 = lax.broadcasted_iota(jnp.int32, (8, 128), 0)
    low_heads = sub8 < 4
    scale = 128 ** -0.5

    def new_rows(buf, b):
        return jnp.where(low_heads, buf[0, pl.ds(b, 1), :], buf[1, pl.ds(b, 1), :])

    def a_rows(g):
        return pl.ds(g * GROUP, GROUP + (2 if g == rows // GROUP - 1 else 0))

    groups = rows // GROUP

    def a_start(g, k):
        remote(part.at[a_rows(g)], part_rx.at[k, a_rows(g)], 0, a_sem.at[k], (0, k + 1)).start()

    m_all = jnp.zeros((8, 128), F32)
    l_all = jnp.zeros((8, 128), F32)
    n_all = jnp.zeros((8, 128), F32)

    def group_scores(g):
        wait_bytes(k_buf.at[pl.ds(0, 2 * GROUP)], k_sem.at[g])
        start_load(W_CHUNKS + FLIGHT + 2 + g)
        return [
            lax.dot_general(
                q_buf[b].astype(BF16), k_buf[b], (((1,), (1,)), ((), ())), preferred_element_type=F32
            )
            for b in range(g * GROUP, (g + 1) * GROUP)
        ]

    pending = group_scores(0)
    for g in range(groups):
        ids = range(g * GROUP, (g + 1) * GROUP)
        scores = pending
        if g + 1 < groups:
            pending = group_scores(g + 1)
        probs = []
        for b, sc in zip(ids, scores):
            fresh = jnp.sum(q_buf[b] * new_rows(kn_buf, b), axis=-1, keepdims=True) * scale
            ploc = pos[b] - first_slot
            mask = own & (slot_id < ploc) & (slot_id >= ploc - WINDOW)
            sc = jnp.where(mask, sc * scale, NEG)
            m = jnp.max(sc, axis=-1, keepdims=True)
            w = jnp.where(mask, jnp.exp(sc - m), 0.0)
            l = jnp.sum(w, axis=-1, keepdims=True)
            at = lane8 == sub8 + b * 8
            n_all = jnp.where(at, fresh, n_all)
            m_all = jnp.where(at, m, m_all)
            l_all = jnp.where(at, l, l_all)
            probs.append(w.astype(BF16))
        for b, w in zip(ids, probs):
            part[b] = jnp.dot(w, v_buf[b], preferred_element_type=F32)
        if g == rows // GROUP - 1:
            part[rows] = m_all
            part[rows + 1] = l_all
        for k in (1, 2, 0):
            a_start(g, k)
        if g == groups - 2:
            start_wo()
    for c in range(4):
        start_wg(c)
    start_wd()

    for k in range(3):
        wait_bytes(part_rx.at[k], a_sem.at[k])
    parts = [part, part_rx.at[0], part_rx.at[1], part_rx.at[2]]
    top = n_all
    for p in parts:
        top = jnp.maximum(top, p[rows])
    facs = [jnp.exp(p[rows] - top) for p in parts]
    fresh = jnp.exp(n_all - top)
    total = fresh
    for p, f in zip(parts, facs):
        total = total + p[rows + 1] * f
    inv = 1.0 / total
    facs = [f * inv for f in facs]
    fresh = fresh * inv
    for b in range(rows):
        at = lane8 == sub8 + b * 8
        o = new_rows(vn_buf, b) * jnp.sum(jnp.where(at, fresh, 0.0), axis=-1, keepdims=True)
        for p, f in zip(parts, facs):
            o = o + p[b] * jnp.sum(jnp.where(at, f, 0.0), axis=-1, keepdims=True)
        o_buf[b] = o
    for h in range(8):
        ob_buf[:, h * 128:(h + 1) * 128] = o_buf[:, h, :].astype(BF16)

    def reduce_scatter(make_term, tx, rx, phase, sem):
        for dts in ((3,), (2, 1, 0)):
            for dt in dts:
                tx[dt] = make_term(t ^ dt)
            for dt in dts:
                remote(tx.at[dt], rx.at[dt], phase, sem, (dt, 1)).start()
        wait_bytes(rx, sem)
        return rx[0] + rx[1] + rx[2] + rx[3]

    wait_bytes(wo_buf, wo_sem)
    o_all = ob_buf[...]

    def out_term(d):
        return jnp.dot(o_all, wo_buf[d], preferred_element_type=F32).astype(BF16).astype(F32)

    my_cols = pl.ds(pl.multiple_of(me * 256, 256), 256)
    mid = x_buf[:, my_cols].astype(F32) + reduce_scatter(out_term, rs_tx, rs_rx, 1, b_sem)
    ag_buf[me] = mid
    sq = jnp.sum(mid * mid, axis=-1, keepdims=True)
    ss_buf[me] = jnp.sum(jnp.where(diag, sq, 0.0), axis=0, keepdims=True)

    class Gather:
        def __init__(self, buf, sems, phase):
            self.buf, self.sems, self.phase = buf, sems, phase

        def send(self, have):
            for off in sorted(OFFSETS, key=lambda o: (o[1] != 3 or o[0] == 0, -o[0])):
                k = OFFSETS.index(off)
                if add_offsets(off, VIA[off]) == have:
                    slot = piece_of(have)
                    recv = self.sems.at[k if k < 8 else 8 + off[1] // 2]
                    remote(self.buf.at[slot], self.buf.at[slot], self.phase, recv, VIA[off]).start()

        def wait(self, off):
            slot = piece_of(off)
            k = OFFSETS.index(off)
            remote(self.buf.at[slot], self.buf.at[slot], self.phase, self.sems.at[k], off).wait_recv()
            self.send(off)

        def wait_block(self, ds):
            wait_bytes(self.buf.at[pl.ds(0, 3 if ds == 0 else 4)], self.sems.at[8 + ds // 2])

    for off in sorted(OFFSETS, key=lambda o: -o[0]):
        remote(ss_buf.at[me], ss_buf.at[me], 2, s_sem, off).start()
    gather = Gather(ag_buf, g_sem, 3)
    gather.send((0, 0))
    for off in OFFSETS[:3]:
        gather.wait(off)
    wait_bytes(ss_buf.at[pl.ds(0, len(OFFSETS))], s_sem)
    tot = jnp.sum(ss_buf[...], axis=0)
    mean_sq = jnp.sum(jnp.where(diag, tot, 0.0), axis=-1, keepdims=True) / dim
    rstd = lax.rsqrt(mean_sq + NORM_EPS)
    wait_bytes(wg_buf, wg_sem)

    def normed(off):
        slot = piece_of(off)
        at = pl.ds(pl.multiple_of(slot * 256, 256), 256)
        return (ag_buf[slot] * rstd * gain2[:, at]).astype(BF16), at

    def gate_up(pieces, cols):
        out = None
        for r2, at in pieces:
            term = jnp.dot(r2, wg_buf[at, cols], preferred_element_type=F32)
            out = term if out is None else out + term
        return out

    whole = slice(0, 2 * units)
    hid = gate_up([normed(off) for off in ((0, 0),) + OFFSETS[:3]], whole)
    for off in OFFSETS[3:8]:
        gather.wait(off)
    hid = hid + gate_up([normed(off) for off in OFFSETS[3:8]], whole)
    gather.wait_block(0)
    gather.wait_block(2)
    late = [normed(off) for off in OFFSETS[8:]]
    acts = (act_a, act_b)
    spans = (slice(0, act_a.shape[2]), slice(act_a.shape[2], units))
    for i in range(2):
        g_cols = spans[i]
        u_cols = slice(units + g_cols.start, units + g_cols.stop)
        gate = hid[:, g_cols] + gate_up(late, g_cols)
        up = hid[:, u_cols] + gate_up(late, u_cols)
        acts[i][core] = (gate * jax.nn.sigmoid(gate) * up).astype(BF16).astype(F32)
        remote(acts[i].at[core], acts[i].at[core], 4 + 4 * i, c_sem.at[i], (0, 1)).start()

    wait_bytes(wd_buf, wd_sem)

    def down_part(i, which):
        return jnp.dot(acts[i][which].astype(BF16), wd_buf[which, spans[i], :], preferred_element_type=F32)

    down = down_part(0, core) + down_part(1, core)
    for i in range(2):
        wait_bytes(acts[i].at[1 - core], c_sem.at[i])
        down = down + down_part(i, 1 - core)
    down = down.astype(BF16).astype(F32)
    for d in range(TP):
        dn_buf[d] = down[:, d * 256:(d + 1) * 256]

    for dt in (3, 2, 1, 0):
        remote(dn_buf.at[t ^ dt], rs2_rx.at[dt], 5, d_sem, (dt, 1)).start()
    wait_bytes(rs2_rx, d_sem)
    ag2_buf[me] = mid + rs2_rx[0] + rs2_rx[1] + rs2_rx[2] + rs2_rx[3]
    gather2 = Gather(ag2_buf, e_sem, 6)
    gather2.send((0, 0))
    for off in OFFSETS[:8]:
        gather2.wait(off)
    gather2.wait_block(0)
    gather2.wait_block(2)
    for i in range(16):
        out_ref[:, i * 256:(i + 1) * 256] = ag2_buf[i]
    sent = (
        part_rx, rs_tx, ss_buf.at[pl.ds(0, 15)], ag_buf.at[pl.ds(0, 15)], act_a.at[0],
        dn_buf, ag2_buf.at[pl.ds(0, 15)], qkv_buf.at[0], act_b.at[0],
    )
    for phase, ref in enumerate(sent):
        wait_bytes(ref, send_sem.at[phase])


def store_kernel(
    pos, x2_ref, kn_ref, vn_ref, k_in, v_in, out_ref, k_out, v_out, k_buf, v_buf, x2, x_sem, k_sem, v_sem
):
    rows, keys = k_out.shape[:2]
    x2[...] = x2_ref[...].astype(BF16)
    out = pltpu.make_async_copy(x2, out_ref, x_sem)
    out.start()
    first_slot = lax.axis_index("sp") * (keys // 2)
    row16 = lax.broadcasted_iota(jnp.int32, (16, 128), 0)

    def put(ref, new, b, ploc):
        start = pl.multiple_of((jnp.clip(ploc * 2, 0, keys - 2) // 16) * 16, 16)
        block = ref[b, pl.ds(start, 16), :].astype(F32)
        at = row16 + start
        block = jnp.where(at == ploc * 2, new[0, b:b + 1, :], block)
        block = jnp.where(at == ploc * 2 + 1, new[1, b:b + 1, :], block)
        ref[b, pl.ds(start, 16), :] = block.astype(BF16)

    for b in range(rows):
        ploc = pos[b] - first_slot
        put(k_buf, kn_ref, b, ploc)
        for h in range(2):
            at = pl.ds(h * (keys // 2), keys // 2)
            pltpu.make_async_copy(k_buf.at[b, at], k_out.at[b, at], k_sem).start()
        put(v_buf, vn_ref, b, ploc)
        for h in range(2):
            at = pl.ds(h * (keys // 2), keys // 2)
            pltpu.make_async_copy(v_buf.at[b, at], v_out.at[b, at], v_sem).start()
    out.wait()
    pltpu.make_async_copy(k_buf, k_out, k_sem).wait()
    pltpu.make_async_copy(v_buf, v_out, v_sem).wait()


def solution(mesh):
    cache_spec = P("dp", "sp", "tp", None)
    vmem = pl.BlockSpec(memory_space=pltpu.VMEM)
    smem = pl.BlockSpec(memory_space=pltpu.SMEM)
    hbm = pl.BlockSpec(memory_space=pltpu.HBM)

    def in_hbm(*arrays):
        return tuple(pltpu.with_memory_space_constraint(a, pltpu.HBM) for a in arrays)

    def local_step(hidden, positions, norm_attn, norm_mlp, w_qkv, w_out, w_gate_up, w_down, k_cache, v_cache):
        rows, block_len, kv_local, head_dim = k_cache.shape
        dim = hidden.shape[1]
        flat = (rows, block_len * kv_local, head_dim)
        freq = ROPE_BASE ** (-np.arange(0, head_dim, 2, dtype=np.float64) / head_dim)
        freq = jnp.asarray(np.concatenate([freq, freq])[None].astype(np.float32))
        units = w_down.shape[0] // 2
        fresh = (kv_local, rows, head_dim)
        x2, k_mid, v_mid, k_new, v_new, pos = pl.pallas_call(
            layer_kernel,
            out_shape=(
                pltpu.VMEM((rows, dim), F32),
                pltpu.VMEM(flat, BF16),
                pltpu.VMEM(flat, BF16),
                pltpu.VMEM(fresh, F32),
                pltpu.VMEM(fresh, F32),
                pltpu.SMEM((rows,), jnp.int32),
            ),
            in_specs=[hbm] * 11,
            out_specs=(vmem,) * 5 + (smem,),
            scratch_shapes=[
                pltpu.VMEM((1, head_dim), F32),
                pltpu.VMEM((rows, dim), BF16),
                pltpu.VMEM((1, dim), F32),
                pltpu.VMEM((1, dim), F32),
                pltpu.VMEM((TP, 1024, 256), BF16),
                pltpu.VMEM((dim, 2 * units), BF16),
                pltpu.VMEM((2, units, 1024), BF16),
                pltpu.VMEM((rows, dim), BF16),
                pltpu.VMEM((2, rows, w_qkv.shape[1] // 2), F32),
                pltpu.VMEM((rows, 8, 128), F32),
                pltpu.VMEM((rows + 2, 8, 128), F32),
                pltpu.VMEM((3, rows + 2, 8, 128), F32),
                pltpu.VMEM((rows, 8, 128), F32),
                pltpu.VMEM((rows, 1024), BF16),
                pltpu.VMEM((TP, rows, 256), F32),
                pltpu.VMEM((TP, rows, 256), F32),
                pltpu.VMEM((16, rows, 256), F32),
                pltpu.VMEM((16, 1, 128), F32),
                pltpu.VMEM((2, rows, 1024), F32),
                pltpu.VMEM((2, rows, units - 1024), F32),
                pltpu.VMEM((TP, rows, 256), F32),
                pltpu.VMEM((TP, rows, 256), F32),
                pltpu.VMEM((16, rows, 256), F32),
                pltpu.SemaphoreType.DMA((5,)),
                pltpu.SemaphoreType.DMA((W_CHUNKS,)),
                pltpu.SemaphoreType.DMA((rows // GROUP,)),
                pltpu.SemaphoreType.DMA,
                pltpu.SemaphoreType.DMA,
                pltpu.SemaphoreType.DMA,
                pltpu.SemaphoreType.DMA((3,)),
                pltpu.SemaphoreType.DMA,
                pltpu.SemaphoreType.DMA,
                pltpu.SemaphoreType.DMA((10,)),
                pltpu.SemaphoreType.DMA((2,)),
                pltpu.SemaphoreType.DMA,
                pltpu.SemaphoreType.DMA((10,)),
                pltpu.SemaphoreType.DMA,
                pltpu.SemaphoreType.DMA((9,)),
            ],
            compiler_params=pltpu.CompilerParams(
                collective_id=0, has_side_effects=True, vmem_limit_bytes=44 * 2 ** 20
            ),
            cost_estimate=pl.CostEstimate(flops=4 * 10 ** 9, bytes_accessed=6 * 10 ** 7, transcendentals=10 ** 6),
        )(*in_hbm(
            positions, freq, hidden, norm_attn.reshape(1, dim), norm_mlp.reshape(1, dim), w_qkv,
            k_cache.reshape(flat), v_cache.reshape(flat), w_out, w_gate_up, w_down,
        ))
        result, k_upd, v_upd, _, _ = pl.pallas_call(
            store_kernel,
            out_shape=(
                jax.ShapeDtypeStruct((rows, dim), BF16),
                jax.ShapeDtypeStruct(flat, BF16),
                jax.ShapeDtypeStruct(flat, BF16),
                pltpu.VMEM(flat, BF16),
                pltpu.VMEM(flat, BF16),
            ),
            in_specs=[smem] + [vmem] * 5,
            out_specs=(hbm, hbm, hbm, vmem, vmem),
            input_output_aliases={4: 3, 5: 4},
            scratch_shapes=[
                pltpu.VMEM((rows, dim), BF16),
                pltpu.SemaphoreType.DMA,
                pltpu.SemaphoreType.DMA,
                pltpu.SemaphoreType.DMA,
            ],
            compiler_params=pltpu.CompilerParams(vmem_limit_bytes=8 * 2 ** 20),
            cost_estimate=pl.CostEstimate(flops=10 ** 8, bytes_accessed=2 * 10 ** 7, transcendentals=0),
        )(pos, x2, k_new, v_new, k_mid, v_mid)
        return result, k_upd.reshape(k_cache.shape), v_upd.reshape(v_cache.shape)

    return jax.shard_map(
        local_step, mesh=mesh,
        in_specs=(P("dp", None), P("dp"), P(None), P(None), P(None, "tp"), P("tp", None), P(None, "tp"), P("tp", None), cache_spec, cache_spec),
        out_specs=(P("dp", None), cache_spec, cache_spec), check_vma=False,
    )
```
